32 devices in a mesh: gx: 4 (over z), yz: 8 (over y, x, core).
Axes of the slice: x: 2, y: 2, z: 4, core: 2. Of those that a mesh axis runs over, the one named last changes fastest.
Arguments:
- positions: bfloat16 [3, 8192], P(None, ('gx', 'yz')), may hold values from 0 to 1
- species: int32 [8192], P(('gx', 'yz')), may hold values from 0 to 5
- features: bfloat16 [8192, 512], P(('gx', 'yz')), may hold values from -6 to 6
- move_dest: int32 [64], P(('gx', 'yz')), may hold values from 0 to 7, as said below
- move_slot: int32 [64], P(('gx', 'yz')), may hold values from 0 to 1, as said below
- halo_list: int32 [1024], P(('gx', 'yz')), may hold values from 0 to 255
- neighbours: int32 [8192, 64], P(('gx', 'yz')), may hold values from 0 to 383, as said below
- neighbour_count: int32 [8192], P(('gx', 'yz')), may hold values from 16 to 64
- wave_index: int32 [3, 4096], replicated, may hold values from -16 to 16, as said below
- radial_in: bfloat16 [8, 64], replicated, may hold values from -2 to 2
- radial_mid: bfloat16 [2, 64, 64], replicated, may hold values from -0.75 to 0.75
- radial_out: bfloat16 [64, 512], replicated, may hold values from -0.75 to 0.75
- up_weight: bfloat16 [2, 128, 128], replicated, may hold values from -0.5 to 0.5
- prod_weight: float32 [6, 640], replicated, may hold values from -4 to 4
- out_weight: bfloat16 [2, 128, 128], replicated, may hold values from -0.5 to 0.5
- skip_weight: bfloat16 [2, 128, 128], replicated, may hold values from -0.5 to 0.5
- charge_weight: bfloat16 [128, 8], replicated, may hold values from -0.5 to 0.5
- field_weight: float32 [8, 128], replicated, may hold values from -2 to 2
- read_weight: bfloat16 [128, 16], replicated, may hold values from -0.5 to 0.5
- read_vector: float32 [16], replicated, may hold values from -1.5 to 1.5
- force_weight: float32 [128], replicated, may hold values from -0.5 to 0.5
Outputs:
- forces: float32 [3, 8192], P(None, ('gx', 'yz'))
- energies: float32 [8192], P(('gx', 'yz'))
The draws below stay inside these ranges and needn't reach their ends.
Inputs may be any that keep to these rules, and one draw needn't show every extreme that they name: `move_dest`: the destination lies in the same gx row. Exactly 2 blocks of each device go to other devices, at most one to any one device, and each device receives exactly 2 blocks; the others stay. `move_slot`: the 2 blocks that a device holds after the move take its 2 slots once each. `neighbours`: row of the device's table: its working atoms, then the ghosts from gx - 1, gx + 1, yz - 1, yz + 1. Never the atom itself; slots from neighbour_count on are padding. `wave_index`: row 0 runs from 1 to 8, row 1 from -16 to 16, row 2 from -2 to 2.
All inputs are finite; a program needn't handle non-finite values.
Results may differ from the reference program's by a relative error of at most 0.0028.
Values may be sent and summed in bfloat16 or wider, within the bound.
A program may use at most 64 MiB of HBM per device.

```python
import math
import jax
import jax.numpy as jnp
from jax import lax

C = 128
Q = 8
K = 4096
NRAD = 8
RAD_H = 64
READ_H = 16
NSPEC = 6
MAXNB = 64
BLK = 128
MOVES = 2
A_DEV = 256
HALO = 32
NB_DEV = 2
DOM_X = 4
DOM_Y = 8
ATOMS = 8192
HALOS = 1024


def shuffled_offsets(subkey):
    return jax.random.permutation(subkey, DOM_Y - 1)[:MOVES].astype(jnp.int32) + 1


def shuffled_blocks(subkey):
    return jax.random.permutation(subkey, NB_DEV).astype(jnp.int32)


def plan_tables(key):
    plan_key = jax.random.fold_in(key, 4242)
    key_offsets, key_order, key_slots = jax.random.split(plan_key, 3)
    devices = DOM_X * DOM_Y
    offsets = jax.vmap(shuffled_offsets)(jax.random.split(key_offsets, DOM_X))
    block_order = jax.vmap(shuffled_blocks)(jax.random.split(key_order, devices))
    slot_order = jax.vmap(shuffled_blocks)(jax.random.split(key_slots, devices))
    device_ids = jnp.arange(devices, dtype=jnp.int32)
    row_of = device_ids // DOM_Y
    column_of = device_ids % DOM_Y
    rounds = jnp.arange(NB_DEV, dtype=jnp.int32)
    padded = jnp.concatenate([offsets, jnp.zeros((DOM_X, NB_DEV - MOVES), jnp.int32)], axis=1)
    dest_round = (column_of[:, None] + padded[row_of]) % DOM_Y
    dest_device = row_of[:, None] * DOM_Y + dest_round
    slot_round = slot_order[dest_device, jnp.broadcast_to(rounds[None, :], dest_device.shape)]
    inverse = jnp.argsort(block_order, axis=1).astype(jnp.int32)
    destination = jnp.take_along_axis(dest_round, inverse, axis=1)
    slot_table = jnp.take_along_axis(slot_round, inverse, axis=1)
    return (destination.reshape(-1).astype(jnp.int32), slot_table.reshape(-1).astype(jnp.int32))


def draw_move_dest(key, part):
    return plan_tables(key)[0]


def draw_move_slot(key, part):
    return plan_tables(key)[1]


def draw_neighbours(key, part):
    table_size = A_DEV + 4 * HALO
    drawn_rows = jax.random.randint(jax.random.fold_in(key, 31), (ATOMS, MAXNB), 0, table_size - 1, dtype=jnp.int32)
    own_row = (jnp.arange(ATOMS, dtype=jnp.int32) % A_DEV)[:, None]
    return drawn_rows + (drawn_rows >= own_row).astype(jnp.int32)


def draw_wave_index(key, part):
    subkeys = jax.random.split(jax.random.fold_in(key, 57), 3)
    along_x = jax.random.randint(subkeys[0], (K,), 1, 2 * DOM_X + 1, dtype=jnp.int32)
    along_y = jax.random.randint(subkeys[1], (K,), -2 * DOM_Y, 2 * DOM_Y + 1, dtype=jnp.int32)
    along_z = jax.random.randint(subkeys[2], (K,), -2, 3, dtype=jnp.int32)
    return jnp.stack([along_x, along_y, along_z])


def place_ends(result, key, low, top_value):
    longest = result.shape.index(max(result.shape))
    spots = []
    for shift in (0, 1):
        where = [jax.random.randint(jax.random.fold_in(key, axis), (), 0, length) for axis, length in enumerate(result.shape)]
        where[longest] = (where[longest] + shift) % result.shape[longest]
        spots.append(tuple(where))
    return result.at[spots[0]].set(low).at[spots[1]].set(top_value)


def steps_of(rng, dims, cuts, low, largest):
    level, own = 1.0, jax.random.fold_in(rng, 6)
    for dim, shards_of in cuts:
        steps = jnp.exp(jax.random.uniform(jax.random.fold_in(own, dim), (shards_of,), jnp.float32, low / len(cuts), largest / len(cuts)))
        level = level * jnp.repeat(steps, dims[dim] // shards_of).reshape([-1 if axis == dim else 1 for axis in range(len(dims))])
    return level


def gaussian(key, extent, spread, bound, cuts=(), held_as=jnp.bfloat16):
    gain = steps_of(key, extent, cuts, -0.22, 0.18) if cuts else 1.0
    values = jax.random.normal(key, extent, jnp.float32) * spread * gain
    return jnp.minimum(jnp.maximum(values, -bound), bound).astype(held_as)


def setup_inputs(seed: int = 0) -> dict:
    keys = jax.random.split(jax.random.key(seed), 22)
    positions = jnp.clip(1.0 * jax.random.uniform(keys[0], (3, ATOMS), jnp.float32) ** steps_of(keys[0], (3, ATOMS), ((1, 32),), -0.2, 0.2), 0.0, 1.0).astype(jnp.bfloat16)
    species = place_ends(jax.random.randint(keys[1], (ATOMS,), 0, NSPEC), jax.random.fold_in(keys[1], 1), 0, NSPEC - 1).astype(jnp.int32)
    features = gaussian(keys[2], (ATOMS, 4 * C), 1.0, 6.0, ((0, 32),))
    move_dest = draw_move_dest(jax.random.fold_in(keys[21], 71), 0)
    move_slot = draw_move_slot(jax.random.fold_in(keys[21], 71), 0)
    halo_list = place_ends(jax.random.randint(keys[5], (HALOS,), 0, A_DEV), jax.random.fold_in(keys[5], 1), 0, A_DEV - 1).astype(jnp.int32)
    neighbours = draw_neighbours(jax.random.fold_in(keys[21], 71), 0)
    neighbour_count = place_ends(jax.random.randint(keys[7], (ATOMS,), MAXNB // 4, MAXNB + 1), jax.random.fold_in(keys[7], 1), MAXNB // 4, MAXNB).astype(jnp.int32)
    wave_index = draw_wave_index(jax.random.fold_in(keys[21], 71), 0)
    radial_in = gaussian(keys[9], (NRAD, RAD_H), NRAD ** -0.5, 2.0)
    radial_mid = gaussian(keys[10], (2, RAD_H, RAD_H), RAD_H ** -0.5, 0.75)
    radial_out = gaussian(keys[11], (RAD_H, 4 * C), RAD_H ** -0.5, 0.75)
    up_weight = gaussian(keys[12], (2, C, C), C ** -0.5, 0.5)
    prod_weight = gaussian(keys[13], (NSPEC, 5 * C), 0.7, 4.0, (), jnp.float32)
    out_weight = gaussian(keys[14], (2, C, C), C ** -0.5, 0.5)
    skip_weight = gaussian(keys[15], (2, C, C), C ** -0.5, 0.5)
    charge_weight = gaussian(keys[16], (C, Q), C ** -0.5, 0.5)
    field_weight = gaussian(keys[17], (Q, C), Q ** -0.5, 2.0, (), jnp.float32)
    read_weight = gaussian(keys[18], (C, READ_H), C ** -0.5, 0.5)
    read_vector = gaussian(keys[19], (READ_H,), READ_H ** -0.5, 1.5, (), jnp.float32)
    force_weight = gaussian(keys[20], (C,), C ** -0.5, 0.5, (), jnp.float32)
    return dict(positions=positions, species=species, features=features, move_dest=move_dest, move_slot=move_slot, halo_list=halo_list, neighbours=neighbours, neighbour_count=neighbour_count, wave_index=wave_index, radial_in=radial_in, radial_mid=radial_mid, radial_out=radial_out, up_weight=up_weight, prod_weight=prod_weight, out_weight=out_weight, skip_weight=skip_weight, charge_weight=charge_weight, field_weight=field_weight, read_weight=read_weight, read_vector=read_vector, force_weight=force_weight)


highest = lax.Precision.HIGHEST
two_pi = 2.0 * math.pi
cutoff_radius = 3.5
basis_sharpness = 4.0
ewald_width = 0.1
ewald_scale = 0.01
atom_step = 64
wave_step = 512

def wave_vectors(wave_index, domains_x, domains_y):
    scales = jnp.array([two_pi / domains_x, two_pi / domains_y, two_pi], jnp.float32)
    wavevectors = wave_index.astype(jnp.float32) * scales[:, None]
    squared = lax.optimization_barrier(jnp.sum(wavevectors * wavevectors, axis=0))
    prefactor = 8.0 * math.pi * ewald_scale / (domains_x * domains_y)
    weights = prefactor * jnp.exp(-0.5 * ewald_width * ewald_width * squared) / squared
    return (wavevectors, weights)

def phase_of(absolute, wavevectors):
    return absolute[0][:, None] * wavevectors[0][None, :] + absolute[1][:, None] * wavevectors[1][None, :] + absolute[2][:, None] * wavevectors[2][None, :]

def structure_terms(absolute, charges, wavevectors):
    stride = math.gcd(wavevectors.shape[1], wave_step)
    block_count = wavevectors.shape[1] // stride

    def one_block(block_index):
        wave_block = lax.dynamic_slice_in_dim(wavevectors, block_index * stride, stride, 1)
        phases = phase_of(absolute, wave_block)
        real_part = jnp.einsum('ak,aq->kq', jnp.cos(phases), charges, precision=highest)
        imag_part = jnp.einsum('ak,aq->kq', jnp.sin(phases), charges, precision=highest)
        return (real_part, imag_part)
    real_part, imag_part = lax.map(one_block, jnp.arange(block_count, dtype=jnp.int32))
    latent = charges.shape[1]
    return (real_part.reshape(-1, latent), imag_part.reshape(-1, latent))

def field_terms(absolute, wavevectors, weights, total_real, total_imag):
    scaled_real = weights[:, None] * total_real
    scaled_imag = weights[:, None] * total_imag
    right_cos = jnp.concatenate([scaled_real] + [-wavevectors[direction][:, None] * scaled_imag for direction in range(3)], axis=1)
    right_sin = jnp.concatenate([scaled_imag] + [wavevectors[direction][:, None] * scaled_real for direction in range(3)], axis=1)
    stride = math.gcd(wavevectors.shape[1], wave_step)
    block_count = wavevectors.shape[1] // stride

    def accumulate(block_index, running):
        wave_block = lax.dynamic_slice_in_dim(wavevectors, block_index * stride, stride, 1)
        phases = phase_of(absolute, wave_block)
        cos_right = lax.dynamic_slice_in_dim(right_cos, block_index * stride, stride, 0)
        sin_right = lax.dynamic_slice_in_dim(right_sin, block_index * stride, stride, 0)
        running = running + jnp.dot(jnp.cos(phases), cos_right, precision=highest)
        return running + jnp.dot(jnp.sin(phases), sin_right, precision=highest)
    initial = jnp.zeros((absolute.shape[1], right_cos.shape[1]), jnp.float32)
    return lax.fori_loop(0, block_count, accumulate, initial)

def project_pair(feature, weights):
    channels = weights.shape[1]
    row_count = feature.shape[0]
    scalar = jnp.dot(feature[:, :channels], weights[0], preferred_element_type=jnp.float32)
    vector = jnp.dot(feature[:, channels:].reshape(row_count * 3, channels), weights[1], preferred_element_type=jnp.float32)
    return jnp.concatenate([scalar, vector.reshape(row_count, 3 * channels)], axis=1)

def edge_products(table_pos, table_up, centre_pos, nbr_rows, nbr_live, coeffs, radial_in, radial_mid, radial_out):
    atom_count, slot_count = nbr_rows.shape
    edge_count = atom_count * slot_count
    flat_rows = nbr_rows.reshape(edge_count)
    offset = (table_pos[:, flat_rows].reshape(3, atom_count, slot_count) - centre_pos[:, :, None]).reshape(3, edge_count)
    distance = jnp.sqrt(lax.optimization_barrier(jnp.sum(offset * offset, axis=0)))
    scaled_dist = distance / cutoff_radius
    envelope = 1.0 - 28.0 * scaled_dist ** 6 + 48.0 * scaled_dist ** 7 - 21.0 * scaled_dist ** 8
    alive_mask = (jnp.arange(slot_count, dtype=jnp.int32)[None, :] < nbr_live[:, None]).astype(jnp.float32).reshape(edge_count)
    basis_count = radial_in.shape[0]
    centres = jnp.arange(basis_count, dtype=jnp.float32) * (cutoff_radius / (basis_count - 1))
    radial_basis = jnp.exp(-basis_sharpness * (distance[:, None] - centres[None, :]) ** 2).astype(jnp.bfloat16)
    hidden = jax.nn.silu(jnp.dot(radial_basis, radial_in, preferred_element_type=jnp.float32)).astype(jnp.bfloat16)
    hidden = jax.nn.silu(jnp.dot(hidden, radial_mid[0], preferred_element_type=jnp.float32)).astype(jnp.bfloat16)
    hidden = jax.nn.silu(jnp.dot(hidden, radial_mid[1], preferred_element_type=jnp.float32)).astype(jnp.bfloat16)
    radial = (jnp.dot(hidden, radial_out, preferred_element_type=jnp.float32) * (envelope * alive_mask)[:, None]).astype(jnp.bfloat16)
    channels = radial.shape[1] // 4
    gathered = table_up[flat_rows]

    def column_block(source, number):
        return source[:, number * channels:(number + 1) * channels].astype(jnp.float32)
    norm_factor = 1.0 / math.sqrt(slot_count)

    def neighbour_sum(values):
        return lax.optimization_barrier(jnp.sum(values.reshape(atom_count, slot_count, channels), axis=1)) * norm_factor
    up_scalar = column_block(gathered, 0)
    up_vector = [column_block(gathered, 1 + direction) for direction in range(3)]
    along = up_vector[0] * offset[0][:, None] + up_vector[1] * offset[1][:, None] + up_vector[2] * offset[2][:, None]
    scalar_msg = neighbour_sum(column_block(radial, 0) * up_scalar + column_block(radial, 1) * along)
    radial_scalar = column_block(radial, 2) * up_scalar
    radial_vector = column_block(radial, 3)
    vector_msg = [neighbour_sum(radial_scalar * offset[direction][:, None] + radial_vector * up_vector[direction]) for direction in range(3)]
    square_sum = vector_msg[0] * vector_msg[0] + vector_msg[1] * vector_msg[1] + vector_msg[2] * vector_msg[2]
    path_weights = [coeffs[:, number * channels:(number + 1) * channels] for number in range(5)]
    scalar_prod = path_weights[0] * scalar_msg + path_weights[1] * scalar_msg * scalar_msg + path_weights[2] * square_sum
    vector_prod = [path_weights[3] * vector_msg[direction] + path_weights[4] * scalar_msg * vector_msg[direction] for direction in range(3)]
    return jnp.concatenate([scalar_prod] + vector_prod, axis=1).astype(jnp.bfloat16)

def atom_results(work_feat, products, charges, efield, out_weight, skip_weight, field_weight, read_weight, read_vector, force_weight):
    channels = out_weight.shape[1]
    latent = charges.shape[1]
    mixed_feat = project_pair(products, out_weight) + project_pair(work_feat, skip_weight)
    potential = efield[:, :latent]
    scalars = mixed_feat[:, :channels] + jnp.dot(potential, field_weight, precision=highest)
    readout = jax.nn.silu(jnp.dot(scalars.astype(jnp.bfloat16), read_weight, preferred_element_type=jnp.float32))
    energy = jnp.dot(readout, read_vector, precision=highest) + 0.5 * lax.optimization_barrier(jnp.sum(charges * potential, axis=1))
    forces = [jnp.dot(mixed_feat[:, (1 + direction) * channels:(2 + direction) * channels], force_weight, precision=highest) + lax.optimization_barrier(jnp.sum(charges * efield[:, (1 + direction) * latent:(2 + direction) * latent], axis=1)) for direction in range(3)]
    return jnp.stack(forces + [energy])

def take_columns(matrix, chosen):
    return matrix[:, chosen]

def take_rows(matrix, chosen):
    return matrix[chosen]

def reference(positions, species, features, move_dest, move_slot, halo_list, neighbours, neighbour_count, wave_index, radial_in, radial_mid, radial_out, up_weight, prod_weight, out_weight, skip_weight, charge_weight, field_weight, read_weight, read_vector, force_weight):
    devices = DOM_X * DOM_Y
    blocks = NB_DEV
    channels = C
    home_device = jnp.arange(devices * blocks, dtype=jnp.int32) // blocks
    target = ((home_device // DOM_Y * DOM_Y + move_dest) * blocks + move_slot).astype(jnp.int32)
    pos_blocks = positions.astype(jnp.float32).reshape(3, devices * blocks, BLK)
    work_pos = jnp.zeros_like(pos_blocks).at[:, target].set(pos_blocks).reshape(3, devices, A_DEV).transpose(1, 0, 2)
    spec_blocks = species.reshape(devices * blocks, BLK)
    work_species = jnp.zeros_like(spec_blocks).at[target].set(spec_blocks).reshape(devices, A_DEV)
    feat_blocks = features.reshape(devices * blocks, BLK, 4 * channels)
    work_feat = jnp.zeros_like(feat_blocks).at[target].set(feat_blocks).reshape(devices, A_DEV, 4 * channels)
    send_lists = halo_list.reshape(devices, HALO)
    send_pos = jax.vmap(take_columns)(work_pos, send_lists).reshape(DOM_X, DOM_Y, 3, HALO)
    send_feat = jax.vmap(take_rows)(work_feat, send_lists).reshape(DOM_X, DOM_Y, HALO, 4 * channels)
    unit_axes = jnp.eye(3, dtype=jnp.float32)
    ghost_pos = [jnp.roll(send_pos, 1, axis=0) - unit_axes[0][:, None], jnp.roll(send_pos, -1, axis=0) + unit_axes[0][:, None], jnp.roll(send_pos, 1, axis=1) - unit_axes[1][:, None], jnp.roll(send_pos, -1, axis=1) + unit_axes[1][:, None]]
    ghost_feat = [jnp.roll(send_feat, 1, axis=0), jnp.roll(send_feat, -1, axis=0), jnp.roll(send_feat, 1, axis=1), jnp.roll(send_feat, -1, axis=1)]
    table_pos = jnp.concatenate([work_pos] + [ghost.reshape(devices, 3, HALO) for ghost in ghost_pos], axis=2)
    table_feat = jnp.concatenate([work_feat] + [ghost.reshape(devices, HALO, 4 * channels) for ghost in ghost_feat], axis=1)
    device_ids = jnp.arange(devices, dtype=jnp.int32)
    anchor = jnp.stack([(device_ids // DOM_Y).astype(jnp.float32), (device_ids % DOM_Y).astype(jnp.float32), jnp.zeros((devices,), jnp.float32)], axis=1)
    absolute = work_pos + anchor[:, :, None]
    charges = jnp.dot(work_feat[:, :, :channels].reshape(devices * A_DEV, channels), charge_weight, preferred_element_type=jnp.float32).reshape(devices, A_DEV, Q)
    wavevectors, weights = wave_vectors(wave_index, DOM_X, DOM_Y)

    def add_device(running, inputs):
        part_real, part_imag = structure_terms(inputs[0], inputs[1], wavevectors)
        return ((running[0] + part_real, running[1] + part_imag), None)
    initial = (jnp.zeros((K, Q), jnp.float32), jnp.zeros((K, Q), jnp.float32))
    (total_real, total_imag), ignored = lax.scan(add_device, initial, (absolute, charges))

    def one_device(inputs):
        tab_pos, tab_feat, own_pos, own_abs, own_species, own_feat, nbr_rows, nbr_live, own_charges = inputs
        table_up = project_pair(tab_feat, up_weight).astype(jnp.bfloat16)
        onehot = (own_species[:, None] == jnp.arange(NSPEC, dtype=jnp.int32)[None, :]).astype(jnp.float32)
        coeffs = jnp.dot(onehot, prod_weight, precision=highest)
        block_count = A_DEV // atom_step

        def edge_block(pieces):
            return edge_products(tab_pos, table_up, pieces[2], pieces[0], pieces[1], pieces[3], radial_in, radial_mid, radial_out)
        products = lax.map(edge_block, (nbr_rows.reshape(block_count, atom_step, MAXNB), nbr_live.reshape(block_count, atom_step), own_pos.reshape(3, block_count, atom_step).transpose(1, 0, 2), coeffs.reshape(block_count, atom_step, 5 * channels))).reshape(A_DEV, 4 * channels)
        efield = field_terms(own_abs, wavevectors, weights, total_real, total_imag)
        return atom_results(own_feat, products, own_charges, efield, out_weight, skip_weight, field_weight, read_weight, read_vector, force_weight)
    results = lax.map(one_device, (table_pos, table_feat, work_pos, absolute, work_species, work_feat, neighbours.reshape(devices, A_DEV, MAXNB), neighbour_count.reshape(devices, A_DEV), charges))
    res_blocks = results.reshape(devices, 4, blocks, BLK).transpose(1, 0, 2, 3).reshape(4, devices * blocks, BLK)
    home_res = res_blocks[:, target].reshape(4, devices * A_DEV)
    return (home_res[:3], home_res[3])
```

```python
import functools
import math

import jax
import jax.numpy as jnp
from jax import lax
from jax.experimental import pallas as pl
from jax.experimental.pallas import tpu as pltpu
from jax.sharding import PartitionSpec as P

highest = lax.Precision.HIGHEST
two_pi = 2.0 * math.pi
cutoff_radius = 3.5
basis_sharpness = 4.0
ewald_width = 0.1
ewald_scale = 0.01
z_reach = 2
lanes = 128
group = 8
f32 = jnp.float32
bf16 = jnp.bfloat16
i32 = jnp.int32

VMEM = pl.BlockSpec(memory_space=pltpu.VMEM)
SMEM = pl.BlockSpec(memory_space=pltpu.SMEM)
MESH = pl.DeviceIdType.MESH
NT = (((1,), (1,)), ((), ()))
TN = (((0,), (0,)), ((), ()))


def nt(a, b, precision=None):
    return lax.dot_general(a, b, NT, precision=precision, preferred_element_type=f32)


def tn(a, b, precision=None):
    return lax.dot_general(a, b, TN, precision=precision, preferred_element_type=f32)


def mm(a, b, precision=None):
    return jnp.dot(a, b, precision=precision, preferred_element_type=f32)


def iota(shape, dim):
    return lax.broadcasted_iota(jnp.int32, shape, dim)


def silu(v):
    half = 0.5 * v
    return half + half * jnp.tanh(half)


def turn_cos_sin(turns):
    frac = turns - jnp.floor(turns + 0.5)
    angle = two_pi * frac
    return jnp.cos(angle), jnp.sin(angle)


def flip(a):
    return a.astype(f32).T.astype(a.dtype)


def step_kernel(
    sizes,
    dest, slot, pos, species, feat, halo, nbr, count, wave, rin, mid, rout, up, prod, ow, sw,
    charge, fieldw, readw, rvec, fw,
    out,
    meta_in, meta_out, meta_got, feat_out, feat_got, work,
    halo_pos, ghost_pos, halo_feat, ghost_feat,
    xz, ymat, dmat, part_out, part_got, row_sum, row_got, coef, coefs,
    nbr_t, rel, hidden, table_t, acc, back, came,
    meta_s, meta_r, feat_s, feat_r, hp_s, hp_r, hf_s, hf_r, rs_s, rs_r, gs_s, gs_r, ag_s, ag_r,
    ret_s, ret_r,
):
    gx, yz, nyp = sizes
    row, me = lax.axis_index("gx"), lax.axis_index("yz")
    atoms, width = feat.shape
    channels = width // 4
    blocks = dest.shape[0]
    block = atoms // blocks
    slots = nbr.shape[1]
    groups = slots // group
    latent = charge.shape[1]
    nx = 2 * gx
    pairs = nx * (2 * z_reach + 1)
    share = pairs * latent // yz
    halos = halo.shape[1]
    width_y = ymat.shape[0]

    def peer(k):
        return lax.rem(me + k, yz)

    def row_peer(k):
        return lax.rem(row + k, gx)

    def to_yz(src, dst, s, r, k):
        return pltpu.make_async_remote_copy(
            src_ref=src, dst_ref=dst, send_sem=s, recv_sem=r,
            device_id={"yz": peer(k)}, device_id_type=MESH,
        )

    def to_gx(src, dst, s, r, k):
        return pltpu.make_async_remote_copy(
            src_ref=src, dst_ref=dst, send_sem=s, recv_sem=r,
            device_id={"gx": row_peer(k)}, device_id_type=MESH,
        )

    barrier = pltpu.get_barrier_semaphore()
    for k in range(1, yz):
        pl.semaphore_signal(barrier, inc=1, device_id={"yz": peer(k)}, device_id_type=MESH)
    for k in range(1, gx):
        pl.semaphore_signal(barrier, inc=1, device_id={"gx": row_peer(k)}, device_id_type=MESH)

    meta_in[...] = jnp.concatenate(
        [pos[...].astype(f32), species[...].astype(f32), jnp.zeros((4, atoms), f32)], axis=0
    )
    line = iota((8, block), 0)
    for d in range(yz):
        picked = jnp.zeros((block, width), bf16)
        record = jnp.zeros((8, block), f32)
        for b in range(blocks):
            cut = slice(b * block, (b + 1) * block)
            hit = jnp.where(jnp.full((1, 1), dest[b], i32) == d, 1.0, 0.0)
            mark = (slot[b] + 1).astype(f32)
            picked = picked + hit.astype(bf16) * feat[cut, :]
            record = record + hit * jnp.where(line == 4, mark, meta_in[:, cut])
        feat_out[d] = picked
        meta_out[d] = record
    pl.semaphore_wait(barrier, yz - 1 + gx - 1)

    meta_copies, feat_copies = [], []
    for k in range(1, yz):
        c = to_yz(meta_out.at[peer(k)], meta_got.at[k], meta_s.at[k], meta_r.at[k], k)
        c.start()
        meta_copies.append(c)
    for k in range(1, yz):
        c = to_yz(feat_out.at[peer(k)], feat_got.at[k], feat_s.at[k], feat_r.at[k], k)
        c.start()
        feat_copies.append(c)
    sent = meta_copies + feat_copies

    for g in range(groups):
        nbr_t[g] = nbr[...].astype(f32).T[g * group : (g + 1) * group, :].astype(i32)
    rin_t = jnp.concatenate([rin[...].astype(f32), jnp.zeros_like(rin, f32)], axis=0).T.astype(bf16)
    mid_t = [flip(mid[i]) for i in range(2)]
    rout_t = flip(rout[...])

    codes = (wave[2:3, :] + z_reach) * nx + wave[0:1, :] - 1
    waves = wave.shape[1]
    hot = ((me * share + iota((share, waves), 0)) // latent == codes).astype(f32).astype(bf16)
    level = iota((nyp, waves), 0)
    plus = (level == wave[1:2, :]).astype(f32).astype(bf16)
    minus = ((level == -wave[1:2, :]) & (level > 0)).astype(f32).astype(bf16)
    pair = (me * share + iota((share, nyp), 0)) // latent
    wx = ((pair % nx) + 1).astype(f32) * (two_pi / gx)
    wz = ((pair // nx) - z_reach).astype(f32) * two_pi
    wy = iota((share, nyp), 1).astype(f32) * (two_pi / yz)
    squared = wx * wx + wy * wy + wz * wz
    prefactor = 8.0 * math.pi * ewald_scale / (gx * yz)
    weight = prefactor * jnp.exp(-0.5 * ewald_width * ewald_width * squared) / squared
    gp, gm = weight * nt(hot, plus), weight * nt(hot, minus)

    for c in meta_copies:
        c.wait_recv()
    meta_got[0] = meta_out[me]
    metas = []
    for s in range(blocks):
        total = jnp.zeros((8, block), f32)
        for k in range(yz):
            got = meta_got[k]
            total = total + jnp.where(got[4:5, :] == s + 1.0, got, 0.0)
        metas.append(total)
    meta = jnp.concatenate(metas, axis=1)

    list4 = jnp.concatenate([halo[...]] * 4, axis=1)
    pick_t = (iota((atoms, 4 * halos), 0) == list4).astype(f32)
    halo_pos[...] = mm(meta.astype(bf16), pick_t.astype(bf16))
    pick = pick_t.T[:halos].astype(bf16)
    ways = ((to_gx, 1, gx), (to_gx, gx - 1, gx), (to_yz, 1, yz), (to_yz, yz - 1, yz))
    ghost_copies = []
    for i, (send, k, n) in enumerate(ways):
        c = send(halo_pos, ghost_pos.at[i], hp_s.at[i], hp_r.at[i], k)
        c.start()
        ghost_copies.append(c)
    sent += ghost_copies

    x_turns = (meta[0:1] + row.astype(f32)) * (1.0 / gx)
    y_turns = (meta[1:2] + me.astype(f32)) * (1.0 / yz)
    xc, xs = turn_cos_sin((iota((nx, atoms), 0) + 1).astype(f32) * x_turns)
    zc, zs = turn_cos_sin((iota((8, atoms), 0) - z_reach).astype(f32) * meta[2:3])
    yc, ys = turn_cos_sin(iota((nyp, atoms), 0).astype(f32) * y_turns)
    for m in range(2 * z_reach + 1):
        c1, s1 = zc[m : m + 1], zs[m : m + 1]
        xz[0, m * nx : (m + 1) * nx, :] = xc * c1 - xs * s1
        xz[1, m * nx : (m + 1) * nx, :] = xc * s1 + xs * c1
    ymat[...] = jnp.zeros_like(ymat)
    dmat[...] = jnp.zeros_like(dmat)
    wide = iota((nyp, atoms), 0).astype(f32) * (two_pi / yz)
    for half in range(2):
        cut = slice(half * atoms, (half + 1) * atoms)
        sign = -1.0 if half == 0 else 1.0
        base = 2 * half * nyp
        ymat[base : base + nyp, cut] = yc
        ymat[base + nyp : base + 2 * nyp, cut] = ys
        dmat[base : base + nyp, cut] = sign * wide * ys
        dmat[base + nyp : base + 2 * nyp, cut] = -sign * wide * yc

    for c in ghost_copies:
        c.wait_recv()
    part = iota((8, 4 * halos), 1) // halos
    lead = iota((8, 4 * halos), 0)
    ghosts = jnp.zeros((8, 4 * halos), f32)
    for i, (axis, shift) in enumerate(((0, -1.0), (0, 1.0), (1, -1.0), (1, 1.0))):
        ghosts = jnp.where(part == i, ghost_pos[i] + jnp.where(lead == axis, shift, 0.0), ghosts)
    table_pos = jnp.concatenate([meta, ghosts], axis=1)
    table = table_pos.shape[1]
    counts = count[...]
    nrad = rin.shape[0]
    centres = iota((2 * nrad, atoms), 0).astype(f32) * (cutoff_radius / (nrad - 1))

    def radial_step(g, carry):
        index = nbr_t[g]
        local = index % lanes
        place = index // lanes
        rs = []
        for m in range(3):
            cols = []
            for h in range(atoms // lanes):
                cut = slice(h * lanes, (h + 1) * lanes)
                found = jnp.zeros((group, lanes), f32)
                for t in range(table // lanes):
                    piece = jnp.broadcast_to(
                        table_pos[m : m + 1, t * lanes : (t + 1) * lanes], (group, lanes)
                    )
                    got = jnp.take_along_axis(piece, local[:, cut], axis=1, mode="promise_in_bounds")
                    found = jnp.where(place[:, cut] == t, got, found)
                cols.append(found)
            r = jnp.concatenate(cols, axis=1) - meta[m : m + 1]
            rel[g, m] = r
            rs.append(r)
        dist = jnp.sqrt(rs[0] * rs[0] + rs[1] * rs[1] + rs[2] * rs[2])
        u = dist * (1.0 / cutoff_radius)
        u2 = u * u
        u6 = u2 * u2 * u2
        env = 1.0 + u6 * (-28.0 + u * (48.0 - 21.0 * u))
        live = (iota((group, atoms), 0) + g * group) < counts
        env = jnp.where(live, env, 0.0)
        basis = []
        for s in range(group):
            off = dist[s : s + 1] - centres
            basis.append(jnp.exp(-basis_sharpness * off * off))
        h = silu(mm(rin_t, jnp.concatenate(basis, axis=1).astype(bf16))).astype(bf16)
        h = silu(mm(mid_t[0], h)).astype(bf16)
        h = silu(mm(mid_t[1], h))
        for s in range(group):
            hidden[g, s] = (h[:, s * atoms : (s + 1) * atoms] * env[s : s + 1]).astype(bf16)
        return carry

    lax.fori_loop(0, groups, radial_step, 0)

    for c in feat_copies:
        c.wait_recv()
    feat_got[0] = feat_out[me]
    for s in range(blocks):
        total = jnp.zeros((block, width), bf16)
        for k in range(yz):
            hit = (meta_got[k, 4:5, 0:1] == s + 1.0).astype(f32).astype(bf16)
            total = total + hit * feat_got[k]
        work[s * block : (s + 1) * block, :] = total
    halo_feat[...] = mm(pick, work[...]).astype(bf16)
    halo_copies = []
    for i, (send, k, n) in enumerate(ways):
        c = send(halo_feat, ghost_feat.at[i], hf_s.at[i], hf_r.at[i], k)
        c.start()
        halo_copies.append(c)
    sent += halo_copies

    scalars = work[:, :channels]
    q = nt(flip(charge[...]), scalars)
    weighted = [
        (xz[i][:, None, :] * q[None]).reshape(pairs * latent, atoms) for i in range(2)
    ]
    part_out[...] = nt(jnp.concatenate(weighted, axis=1), ymat[...], highest).reshape(
        yz, share, width_y
    )
    part_copies = []
    for k in range(1, yz):
        c = to_yz(part_out.at[peer(k)], part_got.at[k], rs_s.at[k], rs_r.at[k], k)
        c.start()
        part_copies.append(c)
    sent += part_copies

    def raise_rows(rows, start, size):
        for p in range(4):
            cut = slice(p * channels, (p + 1) * channels)
            got = mm(rows[:, cut], up[min(p, 1)])
            table_t[cut, start : start + size] = got.T.astype(bf16)

    raise_rows(work[...], 0, atoms)
    for c in halo_copies:
        c.wait_recv()
    raise_rows(
        jnp.concatenate([ghost_feat[i] for i in range(4)], axis=0), atoms, 4 * halos
    )

    acc[...] = jnp.zeros_like(acc)

    def message_step(g, carry):
        index = nbr_t[g]
        r = [rel[g, m] for m in range(3)]
        for s in range(group):
            hot_t = (iota((table, atoms), 0) == index[s : s + 1]).astype(f32).astype(bf16)
            u = mm(table_t[...], hot_t)
            radial = mm(rout_t, hidden[g, s])
            us = [u[p * channels : (p + 1) * channels] for p in range(4)]
            rads = [radial[p * channels : (p + 1) * channels] for p in range(4)]
            rm = [r[m][s : s + 1] for m in range(3)]
            along = rm[0] * us[1] + rm[1] * us[2] + rm[2] * us[3]
            acc[0] += rads[0] * us[0] + rads[1] * along
            ru = rads[2] * us[0]
            for m in range(3):
                acc[1 + m] += ru * rm[m] + rads[3] * us[1 + m]
        return carry

    first, second = groups // 3, 2 * groups // 3
    lax.fori_loop(0, first, message_step, 0)

    for c in part_copies:
        c.wait_recv()
    total = part_out[me]
    for k in range(1, yz):
        total = total + part_got[k]
    row_sum[...] = total
    row_copies = []
    for k in range(1, gx):
        c = to_gx(row_sum, row_got.at[k], gs_s.at[k], gs_r.at[k], k)
        c.start()
        row_copies.append(c)
    sent += row_copies

    lax.fori_loop(first, second, message_step, 0)

    for c in row_copies:
        c.wait_recv()
    total = row_sum[...]
    for k in range(1, gx):
        total = total + row_got[k]
    quarters = [total[:, i * nyp : (i + 1) * nyp] for i in range(4)]
    rest = jnp.zeros((share, width_y - 4 * nyp), f32)
    both, gap = gp + gm, gp - gm
    coef[...] = jnp.concatenate(
        [
            both * quarters[0] - gap * quarters[3],
            both * quarters[1] + gap * quarters[2],
            both * quarters[2] + gap * quarters[1],
            both * quarters[3] - gap * quarters[0],
            rest,
        ],
        axis=1,
    )
    coef_copies = []
    for k in range(1, yz):
        c = to_yz(coef, coefs.at[me], ag_s.at[k], ag_r.at[k], k)
        c.start()
        coef_copies.append(c)
    coefs[me] = coef[...]
    sent += coef_copies

    lax.fori_loop(second, groups, message_step, 0)

    scale = 1.0 / math.sqrt(slots)
    kinds = prod.shape[0]
    kind = meta[3:4]
    which = (iota((8, atoms), 0).astype(f32) == kind).astype(f32).astype(bf16)
    weights = prod[...]
    high = weights.astype(bf16).astype(f32)
    middle = (weights - high).astype(bf16).astype(f32)
    low = weights - high - middle
    gap_rows = jnp.zeros((8 - kinds, weights.shape[1]), f32)
    stack = jnp.concatenate([high, gap_rows, middle, gap_rows, low, gap_rows], axis=0)
    p_t = tn(stack.astype(bf16), jnp.concatenate([which] * 3, axis=0))
    p = [p_t[i * channels : (i + 1) * channels] for i in range(5)]
    a0 = acc[0] * scale
    a1 = [acc[1 + m] * scale for m in range(3)]
    square = a1[0] * a1[0] + a1[1] * a1[1] + a1[2] * a1[2]
    b0 = (p[0] * a0 + p[1] * a0 * a0 + p[2] * square).astype(bf16)
    b1 = [(p[3] * a1[m] + p[4] * a0 * a1[m]).astype(bf16) for m in range(3)]

    for c in coef_copies:
        c.wait_recv()
    full = coefs[...].reshape(yz * share, width_y)
    v = mm(full, ymat[...], highest)
    vy = mm(full, dmat[...], highest)
    v_re, v_im = v[:, :atoms], v[:, atoms:]
    y_im, y_re = vy[:, :atoms], vy[:, atoms:]
    zero = jnp.zeros((latent, atoms), f32)
    potential, field = zero, [zero, zero, zero]
    for j in range(pairs):
        cut = slice(j * latent, (j + 1) * latent)
        cos_row, sin_row = xz[0, j : j + 1], xz[1, j : j + 1]
        d_im = cos_row * v_im[cut] - sin_row * v_re[cut]
        potential = potential + (cos_row * v_re[cut] + sin_row * v_im[cut])
        field[0] = field[0] - ((j % nx) + 1) * (two_pi / gx) * d_im
        field[1] = field[1] - (cos_row * y_im[cut] - sin_row * y_re[cut])
        field[2] = field[2] - ((j // nx) - z_reach) * two_pi * d_im

    scal = (
        tn(ow[0], b0)
        + mm(scalars, sw[0]).T
        + tn(fieldw[...], potential, highest)
    )
    readout = silu(tn(readw[...], scal.astype(bf16)))
    tall = jnp.broadcast_to(rvec[...], (8, rvec.shape[1]))
    energy = mm(tall, readout, highest)[0:1] + 0.5 * jnp.sum(q * potential, axis=0, keepdims=True)
    force8 = jnp.broadcast_to(fw[...], (8, channels))
    to_b = nt(force8, ow[1].astype(f32), highest)
    to_f = nt(force8, sw[1].astype(f32), highest)
    rows = []
    for m in range(3):
        cut = slice((1 + m) * channels, (2 + m) * channels)
        rows.append(
            mm(to_b, b1[m].astype(f32), highest)[0:1]
            + nt(to_f, work[:, cut].astype(f32), highest)[0:1]
            + jnp.sum(q * field[m], axis=0, keepdims=True)
        )
    result = jnp.concatenate(rows + [energy, jnp.zeros((4, atoms), f32)], axis=0)
    for k in range(yz):
        mark = meta_got[k, 4:5, :]
        total = jnp.zeros((8, block), f32)
        for s in range(blocks):
            total = total + jnp.where(mark == s + 1.0, result[:, s * block : (s + 1) * block], 0.0)
        back[k] = total
    back_copies = []
    for k in range(1, yz):
        c = to_yz(back.at[k], came.at[k], ret_s.at[k], ret_r.at[k], yz - k)
        c.start()
        back_copies.append(c)
    sent += back_copies
    for c in back_copies:
        c.wait_recv()
    for b in range(blocks):
        total = jnp.where(dest[b] == me, back[0], jnp.zeros((8, block), f32))
        for k in range(1, yz):
            total = total + jnp.where(dest[b] == peer(k), came[k], jnp.zeros((8, block), f32))
        out[:, b * block : (b + 1) * block] = total
    for c in sent:
        c.wait_send()


def on_device(
    positions,
    species,
    features,
    move_dest,
    move_slot,
    halo_list,
    neighbours,
    neighbour_count,
    wave_index,
    radial_in,
    radial_mid,
    radial_out,
    up_weight,
    prod_weight,
    out_weight,
    skip_weight,
    charge_weight,
    field_weight,
    read_weight,
    read_vector,
    force_weight,
):
    gx, yz = lax.axis_size("gx"), lax.axis_size("yz")
    atoms, width = features.shape
    block = atoms // move_dest.shape[0]
    slots = neighbours.shape[1]
    channels = width // 4
    latent = charge_weight.shape[1]
    nyp = -(-(2 * yz + 1) // 8) * 8
    pairs = 2 * gx * (2 * z_reach + 1)
    share = pairs * latent // yz
    wide = -(-4 * nyp // lanes) * lanes
    halo = halo_list.shape[0]
    groups = slots // group
    table = atoms + 4 * halo
    hidden = radial_mid.shape[1]

    def dma(n):
        return [pltpu.SemaphoreType.DMA((n,)), pltpu.SemaphoreType.DMA((n,))]

    scratch = [
        pltpu.VMEM((8, atoms), f32),
        pltpu.VMEM((yz, 8, block), f32),
        pltpu.VMEM((yz, 8, block), f32),
        pltpu.VMEM((yz, block, width), bf16),
        pltpu.VMEM((yz, block, width), bf16),
        pltpu.VMEM((atoms, width), bf16),
        pltpu.VMEM((8, 4 * halo), f32),
        pltpu.VMEM((4, 8, 4 * halo), f32),
        pltpu.VMEM((halo, width), bf16),
        pltpu.VMEM((4, halo, width), bf16),
        pltpu.VMEM((2, pairs, atoms), f32),
        pltpu.VMEM((wide, 2 * atoms), f32),
        pltpu.VMEM((wide, 2 * atoms), f32),
        pltpu.VMEM((yz, share, wide), f32),
        pltpu.VMEM((yz, share, wide), f32),
        pltpu.VMEM((share, wide), f32),
        pltpu.VMEM((gx, share, wide), f32),
        pltpu.VMEM((share, wide), f32),
        pltpu.VMEM((yz, share, wide), f32),
        pltpu.VMEM((groups, group, atoms), i32),
        pltpu.VMEM((groups, 3, group, atoms), f32),
        pltpu.VMEM((groups, group, hidden, atoms), bf16),
        pltpu.VMEM((width, table), bf16),
        pltpu.VMEM((4, channels, atoms), f32),
        pltpu.VMEM((yz, 8, block), f32),
        pltpu.VMEM((yz, 8, block), f32),
    ]
    scratch += dma(yz) + dma(yz) + dma(4) + dma(4) + dma(yz) + dma(gx) + dma(yz) + dma(yz)
    out = pl.pallas_call(
        functools.partial(step_kernel, (gx, yz, nyp)),
        out_shape=jax.ShapeDtypeStruct((8, atoms), f32),
        in_specs=[SMEM, SMEM] + [VMEM] * 19,
        out_specs=VMEM,
        scratch_shapes=scratch,
        compiler_params=pltpu.CompilerParams(
            collective_id=0, has_side_effects=True, vmem_limit_bytes=56 * 1024 * 1024
        ),
    )(
        move_dest,
        move_slot,
        positions,
        species.reshape(1, atoms),
        features,
        halo_list.reshape(1, halo),
        neighbours,
        neighbour_count.reshape(1, atoms),
        wave_index,
        radial_in,
        radial_mid,
        radial_out,
        up_weight,
        prod_weight,
        out_weight,
        skip_weight,
        charge_weight,
        field_weight,
        read_weight,
        read_vector.reshape(1, -1),
        force_weight.reshape(1, -1),
    )
    return out[:3], out[3]


def solution(mesh):
    split = P(("gx", "yz"))
    rows = P(("gx", "yz"), None)
    in_specs = (P(None, ("gx", "yz")), split, rows, split, split, split, rows, split) + (P(),) * 13
    out_specs = (P(None, ("gx", "yz")), split)
    return jax.shard_map(
        on_device, mesh=mesh, in_specs=in_specs, out_specs=out_specs, check_vma=False
    )
```

```python
import functools
import math

import jax
import jax.numpy as jnp
from jax import lax
from jax.experimental import pallas as pl
from jax.experimental.pallas import tpu as pltpu
from jax.sharding import PartitionSpec as P

highest = lax.Precision.HIGHEST
two_pi = 2.0 * math.pi
cutoff_radius = 3.5
basis_sharpness = 4.0
ewald_width = 0.1
ewald_scale = 0.01
z_reach = 2
lanes = 128
group = 8
f32 = jnp.float32
bf16 = jnp.bfloat16
i32 = jnp.int32

VMEM = pl.BlockSpec(memory_space=pltpu.VMEM)
MESH = pl.DeviceIdType.MESH
NT = (((1,), (1,)), ((), ()))
TN = (((0,), (0,)), ((), ()))


def nt(a, b, precision=None):
    return lax.dot_general(a, b, NT, precision=precision, preferred_element_type=f32)


def tn(a, b, precision=None):
    return lax.dot_general(a, b, TN, precision=precision, preferred_element_type=f32)


def mm(a, b, precision=None):
    return jnp.dot(a, b, precision=precision, preferred_element_type=f32)


def iota(shape, dim):
    return lax.broadcasted_iota(jnp.int32, shape, dim)


def silu(v):
    half = 0.5 * v
    return half + half * jnp.tanh(half)


def turn_cos_sin(turns):
    frac = turns - jnp.floor(turns + 0.5)
    angle = two_pi * frac
    return jnp.cos(angle), jnp.sin(angle)


def flip(a):
    return a.astype(f32).T.astype(a.dtype)


def split(a):
    high = a.astype(bf16)
    return high, (a - high.astype(f32)).astype(bf16)


fields = (
    "dest", "slot", "pos", "species", "feat", "halo", "wave", "nbr", "count", "rin", "mid",
    "rout", "up", "prod", "ow", "sw", "charge", "fieldw", "readw", "rvec", "fw",
)


def step_kernel(sizes, *refs):
    gx, yz, nyp = sizes
    n_in = len(fields)
    sources, refs = refs[:n_in], refs[n_in:]
    forces, energies = refs[:2]
    local, refs = dict(zip(fields, refs[2 : 2 + n_in])), refs[2 + n_in :]
    (
        meta_in, meta_got, spread, pieces, work, halo_pos, ghost_pos, halo_feat, ghost_feat,
        xz, ymat, ypair, part_out, part_got, row_sum, row_got, coef, coefs,
        rel, hidden, radials, table_t, acc, back, came,
        in_s, meta_s, meta_r, sp_s, sp_r, pc_s, pc_r, hp_s, hp_r, hf_s, hf_r, rs_s, rs_r,
        gs_s, gs_r, ag_s, ag_r, ret_s, ret_r,
    ) = refs
    row, me = lax.axis_index("gx"), lax.axis_index("yz")
    blocks, parts, piece, width = local["feat"].shape
    channels = width // 4
    block = parts * piece
    atoms = blocks * block
    slots = local["nbr"].shape[0]
    groups = slots // group
    latent = local["charge"].shape[0]
    nx = 2 * gx
    pairs = nx * (2 * z_reach + 1)
    share = pairs * latent // yz
    halos = local["halo"].shape[1]
    width_y = ymat.shape[0]

    def peer(k):
        return lax.rem(me + k, yz)

    def row_peer(k):
        return lax.rem(row + k, gx)

    def to_yz(src, dst, s, r, k):
        return pltpu.make_async_remote_copy(
            src_ref=src, dst_ref=dst, send_sem=s, recv_sem=r,
            device_id={"yz": peer(k)}, device_id_type=MESH,
        )

    def to_gx(src, dst, s, r, k):
        return pltpu.make_async_remote_copy(
            src_ref=src, dst_ref=dst, send_sem=s, recv_sem=r,
            device_id={"gx": row_peer(k)}, device_id_type=MESH,
        )

    barrier = pltpu.get_barrier_semaphore()
    for k in range(1, yz):
        pl.semaphore_signal(barrier, inc=1, device_id={"yz": peer(k)}, device_id_type=MESH)
    for k in range(1, gx):
        pl.semaphore_signal(barrier, inc=1, device_id={"gx": row_peer(k)}, device_id_type=MESH)
    loads = {}
    for i, name in enumerate(fields):
        loads[name] = pltpu.make_async_copy(sources[i], local[name], in_s.at[i])
        loads[name].start()

    def use(name):
        if name in loads:
            loads.pop(name).wait()
        return local[name]

    dest, slot = use("dest"), use("slot")
    lane = iota((1, atoms), 1)
    place = jnp.zeros((1, atoms), i32)
    spot = jnp.zeros((1, atoms), i32)
    for b in range(blocks):
        code = dest[:, b : b + 1] * blocks + slot[:, b : b + 1]
        place = jnp.where(lane // block == b, code, place)
        spot = jnp.where(lane // piece == me * blocks + b, code * piece + lane % piece, spot)
    meta_in[...] = jnp.concatenate(
        [
            use("pos")[...].astype(f32),
            use("species")[...].astype(f32),
            place.astype(f32),
            spot.astype(f32),
            jnp.zeros((2, atoms), f32),
        ],
        axis=0,
    )
    feat = use("feat")
    pl.semaphore_wait(barrier, yz - 1 + gx - 1)

    sent = []

    def start(copies):
        for c in copies:
            c.start()
        sent.extend(copies)
        return copies

    def arrive(copies):
        for c in copies:
            c.wait_recv()

    others = range(1, yz)
    meta_copies = start(
        [to_yz(meta_in, meta_got.at[k], meta_s.at[k], meta_r.at[k], k) for k in others]
    )
    spread_copies = start(
        [to_yz(feat.at[:, peer(k)], spread.at[me], sp_s.at[k], sp_r.at[k], k) for k in others]
    )

    spread[me] = feat[:, pl.ds(me, 1)].reshape(blocks, piece, width)
    meta_got[0] = meta_in[...]
    wave = use("wave")
    codes = (wave[2:3, :] + z_reach) * nx + wave[0:1, :] - 1
    waves = wave.shape[1]
    hot = ((me * share + iota((share, waves), 0)) // latent == codes).astype(f32).astype(bf16)
    level = iota((nyp, waves), 0)
    plus = (level == wave[1:2, :]).astype(f32).astype(bf16)
    minus = ((level == -wave[1:2, :]) & (level > 0)).astype(f32).astype(bf16)
    pair = (me * share + iota((share, nyp), 0)) // latent
    wx = ((pair % nx) + 1).astype(f32) * (two_pi / gx)
    wz = ((pair // nx) - z_reach).astype(f32) * two_pi
    wy = iota((share, nyp), 1).astype(f32) * (two_pi / yz)
    squared = wx * wx + wy * wy + wz * wz
    prefactor = 8.0 * math.pi * ewald_scale / (gx * yz)
    weight = prefactor * jnp.exp(-0.5 * ewald_width * ewald_width * squared) / squared
    gp, gm = weight * nt(hot, plus), weight * nt(hot, minus)
    rin = use("rin")
    rin_t = jnp.concatenate([rin[...].astype(f32), jnp.zeros_like(rin, f32)], axis=0).T.astype(bf16)
    mid = use("mid")
    mid_t = [flip(mid[i]) for i in range(2)]
    rout_t = flip(use("rout")[...])
    list4 = jnp.concatenate([use("halo")[...]] * 4, axis=1)
    pick_t = (iota((atoms, 4 * halos), 0) == list4).astype(f32)
    pick = pick_t.T[:halos].astype(bf16)
    force8 = jnp.broadcast_to(use("fw")[...], (8, channels))
    ow, sw = use("ow"), use("sw")
    to_b = nt(force8, ow[1].astype(f32), highest)
    to_f = nt(force8, sw[1].astype(f32), highest)
    nbr, counts = use("nbr"), use("count")[...]

    arrive(meta_copies)
    metas = []
    for s in range(blocks):
        mine = (me * blocks + s).astype(f32)
        total = jnp.zeros((8, block), f32)
        for k in range(yz):
            for b in range(blocks):
                got = meta_got[k, :, b * block : (b + 1) * block]
                total = total + jnp.where(got[4:5, :] == mine, got, 0.0)
        metas.append(total)
    meta = jnp.concatenate(metas, axis=1)
    halo_pos[...] = mm(meta.astype(bf16), pick_t.astype(bf16))
    ways = ((to_gx, 1), (to_gx, gx - 1), (to_yz, 1), (to_yz, yz - 1))
    ghost_copies = start(
        [send(halo_pos, ghost_pos.at[i], hp_s.at[i], hp_r.at[i], k) for i, (send, k) in enumerate(ways)]
    )
    targets = meta_got[0, 5:6, :]
    for k in range(1, yz):
        targets = targets + meta_got[k, 5:6, :]
    route = (iota((atoms, atoms), 0).astype(f32) == targets).astype(f32).astype(bf16)

    x_turns = (meta[0:1] + row.astype(f32)) * (1.0 / gx)
    y_turns = (meta[1:2] + me.astype(f32)) * (1.0 / yz)
    xc, xs = turn_cos_sin((iota((nx, atoms), 0) + 1).astype(f32) * x_turns)
    zc, zs = turn_cos_sin((iota((8, atoms), 0) - z_reach).astype(f32) * meta[2:3])
    yc, ys = turn_cos_sin(iota((nyp, atoms), 0).astype(f32) * y_turns)
    for m in range(2 * z_reach + 1):
        c1, s1 = zc[m : m + 1], zs[m : m + 1]
        xz[0, m * nx : (m + 1) * nx, :] = xc * c1 - xs * s1
        xz[1, m * nx : (m + 1) * nx, :] = xc * s1 + xs * c1
    ymat[...] = jnp.zeros_like(ymat)
    rise = iota((nyp, atoms), 0).astype(f32) * (two_pi / yz)
    for half in range(2):
        cut = slice(half * atoms, (half + 1) * atoms)
        far = slice((2 + half) * atoms, (3 + half) * atoms)
        sign = -1.0 if half == 0 else 1.0
        base = 2 * half * nyp
        ymat[base : base + nyp, cut] = yc
        ymat[base + nyp : base + 2 * nyp, cut] = ys
        ymat[base : base + nyp, far] = sign * rise * ys
        ymat[base + nyp : base + 2 * nyp, far] = -sign * rise * yc
    high, low = split(ymat[...])
    ypair[:width_y, :] = high
    ypair[width_y:, :] = low

    arrive(spread_copies)
    pieces[...] = (
        mm(route, spread[...].reshape(atoms, width)).astype(bf16).reshape(yz, blocks, piece, width)
    )
    piece_copies = start(
        [to_yz(pieces.at[peer(k)], work.at[:, me], pc_s.at[k], pc_r.at[k], k) for k in others]
    )
    work[:, pl.ds(me, 1)] = pieces[me].reshape(blocks, 1, piece, width)

    arrive(ghost_copies)
    part = iota((8, 4 * halos), 1) // halos
    lead = iota((8, 4 * halos), 0)
    ghosts = jnp.zeros((8, 4 * halos), f32)
    for i, (axis, shift) in enumerate(((0, -1.0), (0, 1.0), (1, -1.0), (1, 1.0))):
        ghosts = jnp.where(part == i, ghost_pos[i] + jnp.where(lead == axis, shift, 0.0), ghosts)
    table_pos = jnp.concatenate([meta, ghosts], axis=1)
    table = table_pos.shape[1]
    nrad = rin.shape[0]
    centres = iota((2 * nrad, atoms), 0).astype(f32) * (cutoff_radius / (nrad - 1))

    def radial_step(g, carry):
        index = nbr[pl.ds(pl.multiple_of(g * group, group), group), :]
        local_index = index % lanes
        where = index // lanes
        rs = []
        for m in range(3):
            cols = []
            for h in range(atoms // lanes):
                cut = slice(h * lanes, (h + 1) * lanes)
                found = jnp.zeros((group, lanes), f32)
                for t in range(table // lanes):
                    tile = jnp.broadcast_to(
                        table_pos[m : m + 1, t * lanes : (t + 1) * lanes], (group, lanes)
                    )
                    got = jnp.take_along_axis(
                        tile, local_index[:, cut], axis=1, mode="promise_in_bounds"
                    )
                    found = jnp.where(where[:, cut] == t, got, found)
                cols.append(found)
            r = jnp.concatenate(cols, axis=1) - meta[m : m + 1]
            rel[g, m] = r
            rs.append(r)
        dist = jnp.sqrt(rs[0] * rs[0] + rs[1] * rs[1] + rs[2] * rs[2])
        u = dist * (1.0 / cutoff_radius)
        u2 = u * u
        u6 = u2 * u2 * u2
        env = 1.0 + u6 * (-28.0 + u * (48.0 - 21.0 * u))
        live = (iota((group, atoms), 0) + g * group) < counts
        env = jnp.where(live, env, 0.0)
        basis = []
        for s in range(group):
            off = dist[s : s + 1] - centres
            basis.append(jnp.exp(-basis_sharpness * off * off))
        h = silu(mm(rin_t, jnp.concatenate(basis, axis=1).astype(bf16))).astype(bf16)
        h = silu(mm(mid_t[0], h)).astype(bf16)
        h = silu(mm(mid_t[1], h))
        for s in range(group):
            hidden[g, s] = (h[:, s * atoms : (s + 1) * atoms] * env[s : s + 1]).astype(bf16)
        return carry

    lax.fori_loop(0, groups, radial_step, 0)

    arrive(piece_copies)
    owned = work[...].reshape(atoms, width)
    halo_feat[...] = mm(pick, owned).astype(bf16)
    halo_copies = start(
        [send(halo_feat, ghost_feat.at[i], hf_s.at[i], hf_r.at[i], k) for i, (send, k) in enumerate(ways)]
    )

    scalars = owned[:, :channels]
    q = nt(use("charge")[...], scalars)
    weighted = [
        (xz[i][:, None, :] * q[None]).reshape(pairs * latent, atoms) for i in range(2)
    ]
    high, low = split(jnp.concatenate(weighted, axis=1))
    cut = slice(0, 2 * atoms)
    wide = nt(high, ypair[:, cut])
    part_out[...] = (
        wide[:, :width_y] + wide[:, width_y:] + nt(low, ypair[:width_y, cut])
    ).reshape(yz, share, width_y)
    part_copies = start(
        [to_yz(part_out.at[peer(k)], part_got.at[k], rs_s.at[k], rs_r.at[k], k) for k in others]
    )

    up = use("up")

    def raise_rows(rows, begin, size):
        for p in range(4):
            cut = slice(p * channels, (p + 1) * channels)
            got = mm(rows[:, cut], up[min(p, 1)])
            table_t[cut, begin : begin + size] = got.T.astype(bf16)

    raise_rows(owned, 0, atoms)

    skip = mm(scalars, sw[0]).T
    pulls = [
        nt(to_f, owned[:, (1 + m) * channels : (2 + m) * channels].astype(f32), highest)[0:1]
        for m in range(3)
    ]
    prod = use("prod")
    kinds = prod.shape[0]
    which = (iota((8, atoms), 0).astype(f32) == meta[3:4]).astype(f32).astype(bf16)
    weights = prod[...]
    high = weights.astype(bf16).astype(f32)
    middle = (weights - high).astype(bf16).astype(f32)
    low = weights - high - middle
    blank = jnp.zeros((8 - kinds, weights.shape[1]), f32)
    stack = jnp.concatenate([high, blank, middle, blank, low, blank], axis=0)
    p_t = tn(stack.astype(bf16), jnp.concatenate([which] * 3, axis=0))

    def spread_step(g, carry):
        for s in range(group):
            radials[g, s] = mm(rout_t, hidden[g, s]).astype(bf16)
        return carry

    lax.fori_loop(0, groups, spread_step, 0)
    acc[...] = jnp.zeros_like(acc)
    arrive(halo_copies)
    raise_rows(jnp.concatenate([ghost_feat[i] for i in range(4)], axis=0), atoms, 4 * halos)

    def message_step(g, carry):
        index = nbr[pl.ds(pl.multiple_of(g * group, group), group), :]
        r = [rel[g, m] for m in range(3)]
        for s in range(group):
            hot_t = (iota((table, atoms), 0) == index[s : s + 1]).astype(f32).astype(bf16)
            u = mm(table_t[...], hot_t)
            us = [u[p * channels : (p + 1) * channels] for p in range(4)]
            rads = [
                radials[g, s, p * channels : (p + 1) * channels, :].astype(f32) for p in range(4)
            ]
            rm = [r[m][s : s + 1] for m in range(3)]
            along = rm[0] * us[1] + rm[1] * us[2] + rm[2] * us[3]
            acc[0] += rads[0] * us[0] + rads[1] * along
            ru = rads[2] * us[0]
            for m in range(3):
                acc[1 + m] += ru * rm[m] + rads[3] * us[1 + m]
        return carry

    first, second = groups // 4, 5 * groups // 8
    lax.fori_loop(0, first, message_step, 0)

    arrive(part_copies)
    total = part_out[me]
    for k in range(1, yz):
        total = total + part_got[k]
    row_sum[...] = total
    row_copies = start(
        [to_gx(row_sum, row_got.at[k], gs_s.at[k], gs_r.at[k], k) for k in range(1, gx)]
    )

    lax.fori_loop(first, second, message_step, 0)

    arrive(row_copies)
    total = row_sum[...]
    for k in range(1, gx):
        total = total + row_got[k]
    quarters = [total[:, i * nyp : (i + 1) * nyp] for i in range(4)]
    rest = jnp.zeros((share, width_y - 4 * nyp), f32)
    both, gap = gp + gm, gp - gm
    coef[...] = jnp.concatenate(
        [
            both * quarters[0] - gap * quarters[3],
            both * quarters[1] + gap * quarters[2],
            both * quarters[2] + gap * quarters[1],
            both * quarters[3] - gap * quarters[0],
            rest,
        ],
        axis=1,
    )
    coef_copies = start(
        [to_yz(coef, coefs.at[me], ag_s.at[k], ag_r.at[k], k) for k in others]
    )
    coefs[me] = coef[...]

    lax.fori_loop(second, groups, message_step, 0)

    arrive(coef_copies)
    high, low = split(coefs[...].reshape(yz * share, width_y))
    v = mm(jnp.concatenate([high, high], axis=1), ypair[...]) + mm(low, ypair[:width_y, :])
    v_re, v_im, y_im, y_re = [v[:, i * atoms : (i + 1) * atoms] for i in range(4)]
    zero = jnp.zeros((latent, atoms), f32)
    potential, field = zero, [zero, zero, zero]
    for j in range(pairs):
        cut = slice(j * latent, (j + 1) * latent)
        cos_row, sin_row = xz[0, j : j + 1], xz[1, j : j + 1]
        d_im = cos_row * v_im[cut] - sin_row * v_re[cut]
        potential = potential + (cos_row * v_re[cut] + sin_row * v_im[cut])
        field[0] = field[0] - ((j % nx) + 1) * (two_pi / gx) * d_im
        field[1] = field[1] - (cos_row * y_im[cut] - sin_row * y_re[cut])
        field[2] = field[2] - ((j // nx) - z_reach) * two_pi * d_im

    scale = 1.0 / math.sqrt(slots)
    p = [p_t[i * channels : (i + 1) * channels] for i in range(5)]
    a0 = acc[0] * scale
    a1 = [acc[1 + m] * scale for m in range(3)]
    square = a1[0] * a1[0] + a1[1] * a1[1] + a1[2] * a1[2]
    b0 = (p[0] * a0 + p[1] * a0 * a0 + p[2] * square).astype(bf16)
    b1 = [(p[3] * a1[m] + p[4] * a0 * a1[m]).astype(bf16) for m in range(3)]
    scal = tn(ow[0], b0) + skip + tn(use("fieldw")[...], potential, highest)
    readout = silu(mm(use("readw")[...], scal.astype(bf16)))
    rvec = use("rvec")
    tall = jnp.broadcast_to(rvec[...], (8, rvec.shape[1]))
    energy = mm(tall, readout, highest)[0:1] + 0.5 * jnp.sum(q * potential, axis=0, keepdims=True)
    rows = []
    for m in range(3):
        rows.append(
            mm(to_b, b1[m].astype(f32), highest)[0:1]
            + pulls[m]
            + jnp.sum(q * field[m], axis=0, keepdims=True)
        )
    result = jnp.concatenate(rows + [energy, jnp.zeros((4, atoms), f32)], axis=0)
    for k in range(yz):
        for b in range(blocks):
            cut = slice(b * block, (b + 1) * block)
            code = meta_got[k, 4:5, cut]
            total = jnp.zeros((8, block), f32)
            for s in range(blocks):
                mine = (me * blocks + s).astype(f32)
                total = total + jnp.where(
                    code == mine, result[:, s * block : (s + 1) * block], 0.0
                )
            back[k, :, cut] = total
    back_copies = start(
        [to_yz(back.at[k], came.at[k], ret_s.at[k], ret_r.at[k], yz - k) for k in others]
    )
    arrive(back_copies)
    total = back[0]
    for k in range(1, yz):
        total = total + came[k]
    forces[...] = total[:3]
    energies[...] = total[3:4]
    for c in sent:
        c.wait_send()
    assert not loads


def on_device(
    positions,
    species,
    features,
    move_dest,
    move_slot,
    halo_list,
    neighbours,
    neighbour_count,
    wave_index,
    radial_in,
    radial_mid,
    radial_out,
    up_weight,
    prod_weight,
    out_weight,
    skip_weight,
    charge_weight,
    field_weight,
    read_weight,
    read_vector,
    force_weight,
):
    gx, yz = lax.axis_size("gx"), lax.axis_size("yz")
    atoms, width = features.shape
    blocks = move_dest.shape[0]
    piece = atoms // blocks // yz
    slots = neighbours.shape[1]
    channels = width // 4
    latent = charge_weight.shape[1]
    nyp = -(-(2 * yz + 1) // 8) * 8
    pairs = 2 * gx * (2 * z_reach + 1)
    share = pairs * latent // yz
    wide = -(-4 * nyp // lanes) * lanes
    halo = halo_list.shape[0]
    groups = slots // group
    table = atoms + 4 * halo
    hidden = radial_mid.shape[1]

    given = {
        "dest": move_dest.reshape(1, -1),
        "slot": move_slot.reshape(1, -1),
        "pos": positions,
        "species": species.reshape(1, -1),
        "feat": features.reshape(blocks, yz, piece, width),
        "halo": halo_list.reshape(1, -1),
        "wave": wave_index,
        "nbr": neighbours.T,
        "count": neighbour_count.reshape(1, -1),
        "rin": radial_in,
        "mid": radial_mid,
        "rout": radial_out,
        "up": up_weight,
        "prod": prod_weight,
        "ow": out_weight,
        "sw": skip_weight,
        "charge": charge_weight.T,
        "fieldw": field_weight,
        "readw": read_weight.T,
        "rvec": read_vector.reshape(1, -1),
        "fw": force_weight.reshape(1, -1),
    }

    def dma(n):
        return [pltpu.SemaphoreType.DMA((n,)), pltpu.SemaphoreType.DMA((n,))]

    scratch = [pltpu.VMEM(given[name].shape, given[name].dtype) for name in fields]
    scratch += [
        pltpu.VMEM((8, atoms), f32),
        pltpu.VMEM((yz, 8, atoms), f32),
        pltpu.VMEM((yz, blocks, piece, width), bf16),
        pltpu.VMEM((yz, blocks, piece, width), bf16),
        pltpu.VMEM((blocks, yz, piece, width), bf16),
        pltpu.VMEM((8, 4 * halo), f32),
        pltpu.VMEM((4, 8, 4 * halo), f32),
        pltpu.VMEM((halo, width), bf16),
        pltpu.VMEM((4, halo, width), bf16),
        pltpu.VMEM((2, pairs, atoms), f32),
        pltpu.VMEM((wide, 4 * atoms), f32),
        pltpu.VMEM((2 * wide, 4 * atoms), bf16),
        pltpu.VMEM((yz, share, wide), f32),
        pltpu.VMEM((yz, share, wide), f32),
        pltpu.VMEM((share, wide), f32),
        pltpu.VMEM((gx, share, wide), f32),
        pltpu.VMEM((share, wide), f32),
        pltpu.VMEM((yz, share, wide), f32),
        pltpu.VMEM((groups, 3, group, atoms), f32),
        pltpu.VMEM((groups, group, hidden, atoms), bf16),
        pltpu.VMEM((groups, group, width, atoms), bf16),
        pltpu.VMEM((width, table), bf16),
        pltpu.VMEM((4, channels, atoms), f32),
        pltpu.VMEM((yz, 8, atoms), f32),
        pltpu.VMEM((yz, 8, atoms), f32),
    ]
    scratch += [pltpu.SemaphoreType.DMA((len(fields),))]
    scratch += dma(yz) + dma(yz) + dma(yz) + dma(4) + dma(4) + dma(yz) + dma(gx) + dma(yz) + dma(yz)
    forces, energies = pl.pallas_call(
        functools.partial(step_kernel, (gx, yz, nyp)),
        out_shape=[
            jax.ShapeDtypeStruct((3, atoms), f32),
            jax.ShapeDtypeStruct((1, atoms), f32),
        ],
        in_specs=[pl.BlockSpec(memory_space=pl.ANY)] * len(fields),
        out_specs=[VMEM, VMEM],
        scratch_shapes=scratch,
        compiler_params=pltpu.CompilerParams(
            collective_id=0, has_side_effects=True, vmem_limit_bytes=56 * 1024 * 1024
        ),
    )(*[given[name] for name in fields])
    return forces, energies.reshape(atoms)


def solution(mesh):
    split = P(("gx", "yz"))
    rows = P(("gx", "yz"), None)
    in_specs = (P(None, ("gx", "yz")), split, rows, split, split, split, rows, split) + (P(),) * 13
    out_specs = (P(None, ("gx", "yz")), split)
    return jax.shard_map(
        on_device, mesh=mesh, in_specs=in_specs, out_specs=out_specs, check_vma=False
    )
```

```python
import functools
import math

import jax
import jax.numpy as jnp
from jax import lax
from jax.experimental import pallas as pl
from jax.experimental.pallas import tpu as pltpu
from jax.sharding import PartitionSpec as P

highest = lax.Precision.HIGHEST
two_pi = 2.0 * math.pi
cutoff_radius = 3.5
basis_sharpness = 4.0
ewald_width = 0.1
ewald_scale = 0.01
z_reach = 2
lanes = 128
group = 8
together = 2
f32 = jnp.float32
bf16 = jnp.bfloat16
i32 = jnp.int32

VMEM = pl.BlockSpec(memory_space=pltpu.VMEM)
MESH = pl.DeviceIdType.MESH
NT = (((1,), (1,)), ((), ()))
TN = (((0,), (0,)), ((), ()))


def nt(a, b, precision=None):
    return lax.dot_general(a, b, NT, precision=precision, preferred_element_type=f32)


def tn(a, b, precision=None):
    return lax.dot_general(a, b, TN, precision=precision, preferred_element_type=f32)


def mm(a, b, precision=None):
    return jnp.dot(a, b, precision=precision, preferred_element_type=f32)


def iota(shape, dim):
    return lax.broadcasted_iota(jnp.int32, shape, dim)


def silu(v):
    half = 0.5 * v
    return half + half * jnp.tanh(half)


def turn_cos_sin(turns):
    frac = turns - jnp.floor(turns + 0.5)
    angle = two_pi * frac
    return jnp.cos(angle), jnp.sin(angle)


def flip(a):
    return a.astype(f32).T.astype(a.dtype)


def split(a):
    high = a.astype(bf16)
    return high, (a - high.astype(f32)).astype(bf16)


def interleave(parts):
    tall = parts[0].shape[0]
    return jnp.concatenate([p[c : c + 8] for c in range(0, tall, 8) for p in parts], axis=0)


fields = (
    "dest", "slot", "pos", "species", "feat", "halo", "wave", "nbr", "count", "rin", "mid",
    "rout", "up", "prod", "ow", "sw", "charge", "fieldw", "readw", "rvec", "fw",
)


def step_kernel(sizes, *refs):
    gx, yz, nyp = sizes
    n_in = len(fields)
    sources, refs = refs[:n_in], refs[n_in:]
    out, refs = refs[0], refs[1:]
    local, refs = dict(zip(fields, refs[:n_in])), refs[n_in:]
    (
        meta_in, meta_got, spread, pieces, work, halo_pos, ghost_pos, halo_feat, ghost_feat,
        xz, ymat, ypair, part_out, part_got, row_sum, row_got, coef, coefs,
        rel, hidden, radials, hots, table_t, acc, back, came,
        in_s, meta_s, meta_r, sp_s, sp_r, pc_s, pc_r, hp_s, hp_r, hf_s, hf_r, rs_s, rs_r,
        gs_s, gs_r, ag_s, ag_r, ret_s, ret_r,
    ) = refs
    row, me = lax.axis_index("gx"), lax.axis_index("yz")
    blocks, parts, piece, width = local["feat"].shape
    channels = width // 4
    block = parts * piece
    atoms = blocks * block
    slots = local["nbr"].shape[0]
    groups = slots // group
    latent = local["charge"].shape[0]
    nx = 2 * gx
    pairs = nx * (2 * z_reach + 1)
    share = pairs * latent // yz
    halos = local["halo"].shape[1]
    width_y = ymat.shape[0]

    def peer(k):
        return lax.rem(me + k, yz)

    def row_peer(k):
        return lax.rem(row + k, gx)

    def to_yz(src, dst, s, r, k):
        return pltpu.make_async_remote_copy(
            src_ref=src, dst_ref=dst, send_sem=s, recv_sem=r,
            device_id={"yz": peer(k)}, device_id_type=MESH,
        )

    def to_gx(src, dst, s, r, k):
        return pltpu.make_async_remote_copy(
            src_ref=src, dst_ref=dst, send_sem=s, recv_sem=r,
            device_id={"gx": row_peer(k)}, device_id_type=MESH,
        )

    barrier = pltpu.get_barrier_semaphore()
    for k in range(1, yz):
        pl.semaphore_signal(barrier, inc=1, device_id={"yz": peer(k)}, device_id_type=MESH)
    for k in range(1, gx):
        pl.semaphore_signal(barrier, inc=1, device_id={"gx": row_peer(k)}, device_id_type=MESH)
    loads = {}
    for i, name in enumerate(fields):
        loads[name] = pltpu.make_async_copy(sources[i], local[name], in_s.at[i])
        loads[name].start()

    def use(name):
        if name in loads:
            loads.pop(name).wait()
        return local[name]

    dest, slot = use("dest"), use("slot")
    lane = iota((1, atoms), 1)
    place = jnp.zeros((1, atoms), i32)
    spot = jnp.zeros((1, atoms), i32)
    for b in range(blocks):
        code = dest[:, b : b + 1] * blocks + slot[:, b : b + 1]
        place = jnp.where(lane // block == b, code, place)
        spot = jnp.where(lane // piece == me * blocks + b, code * piece + lane % piece, spot)
    meta_in[...] = jnp.concatenate(
        [
            use("pos")[...].astype(f32),
            use("species")[...].astype(f32),
            place.astype(f32),
            spot.astype(f32),
            jnp.zeros((2, atoms), f32),
        ],
        axis=0,
    )
    feat = use("feat")
    pl.semaphore_wait(barrier, yz - 1 + gx - 1)

    sent = []

    def start(copies):
        for c in copies:
            c.start()
        sent.extend(copies)
        return copies

    def arrive(copies):
        for c in copies:
            c.wait_recv()

    others = range(1, yz)
    meta_copies = start(
        [to_yz(meta_in, meta_got.at[k], meta_s.at[k], meta_r.at[k], k) for k in others]
    )
    spread_copies = start(
        [to_yz(feat.at[:, peer(k)], spread.at[me], sp_s.at[k], sp_r.at[k], k) for k in others]
    )

    spread[me] = feat[:, pl.ds(me, 1)].reshape(blocks, piece, width)
    meta_got[0] = meta_in[...]
    wave = use("wave")
    codes = (wave[2:3, :] + z_reach) * nx + wave[0:1, :] - 1
    waves = wave.shape[1]
    hot = ((me * share + iota((share, waves), 0)) // latent == codes).astype(f32).astype(bf16)
    level = iota((nyp, waves), 0)
    plus = (level == wave[1:2, :]).astype(f32).astype(bf16)
    minus = ((level == -wave[1:2, :]) & (level > 0)).astype(f32).astype(bf16)
    pair = (me * share + iota((share, nyp), 0)) // latent
    wx = ((pair % nx) + 1).astype(f32) * (two_pi / gx)
    wz = ((pair // nx) - z_reach).astype(f32) * two_pi
    wy = iota((share, nyp), 1).astype(f32) * (two_pi / yz)
    squared = wx * wx + wy * wy + wz * wz
    prefactor = 8.0 * math.pi * ewald_scale / (gx * yz)
    weight = prefactor * jnp.exp(-0.5 * ewald_width * ewald_width * squared) / squared
    gp, gm = weight * nt(hot, plus), weight * nt(hot, minus)
    rin = use("rin")
    rin_t = jnp.concatenate([rin[...].astype(f32), jnp.zeros_like(rin, f32)], axis=0).T.astype(bf16)
    mid = use("mid")
    mid_t = [flip(mid[i]) for i in range(2)]
    tall = use("rout")[...].astype(f32).T
    rout_t = interleave([tall[p * channels : (p + 1) * channels] for p in range(4)]).astype(bf16)
    list4 = jnp.concatenate([use("halo")[...]] * 4, axis=1)
    pick_t = (iota((atoms, 4 * halos), 0) == list4).astype(f32)
    pick = pick_t.T[:halos].astype(bf16)
    force8 = jnp.broadcast_to(use("fw")[...], (8, channels))
    ow, sw = use("ow"), use("sw")
    to_b = nt(force8, ow[1].astype(f32), highest)
    to_f = nt(force8, sw[1].astype(f32), highest)
    nbr, counts = use("nbr"), use("count")[...]

    packed = 16
    base = iota((packed, atoms), 0).astype(f32).astype(bf16)
    one, nil = jnp.ones((packed, atoms), bf16), jnp.zeros((packed, atoms), bf16)

    def hot_of(index):
        near = jnp.broadcast_to(index, (packed, atoms)).astype(f32)
        far = (near - atoms).astype(bf16)
        near = near.astype(bf16)
        tiles = [jnp.where(near - t == base, one, nil) for t in range(0, atoms, packed)]
        tiles += [jnp.where(far - t == base, one, nil) for t in range(0, 4 * halos, packed)]
        return jnp.concatenate(tiles, axis=0)

    def hot_step(g, carry):
        index = nbr[pl.ds(pl.multiple_of(g * group, group), group), :]
        for s in range(group):
            hots[g, s] = hot_of(index[s : s + 1])
        return carry

    lax.fori_loop(0, groups, hot_step, 0)

    arrive(meta_copies)
    metas = []
    for s in range(blocks):
        mine = (me * blocks + s).astype(f32)
        total = jnp.zeros((8, block), f32)
        for k in range(yz):
            for b in range(blocks):
                got = meta_got[k, :, b * block : (b + 1) * block]
                total = total + jnp.where(got[4:5, :] == mine, got, 0.0)
        metas.append(total)
    meta = jnp.concatenate(metas, axis=1)
    halo_pos[...] = mm(meta.astype(bf16), pick_t.astype(bf16))
    ways = ((to_gx, 1), (to_gx, gx - 1), (to_yz, 1), (to_yz, yz - 1))
    ghost_copies = start(
        [send(halo_pos, ghost_pos.at[i], hp_s.at[i], hp_r.at[i], k) for i, (send, k) in enumerate(ways)]
    )
    targets = meta_got[0, 5:6, :]
    for k in range(1, yz):
        targets = targets + meta_got[k, 5:6, :]
    route = (iota((atoms, atoms), 0).astype(f32) == targets).astype(f32).astype(bf16)

    x_turns = (meta[0:1] + row.astype(f32)) * (1.0 / gx)
    y_turns = (meta[1:2] + me.astype(f32)) * (1.0 / yz)
    xc, xs = turn_cos_sin((iota((nx, atoms), 0) + 1).astype(f32) * x_turns)
    zc, zs = turn_cos_sin((iota((8, atoms), 0) - z_reach).astype(f32) * meta[2:3])
    yc, ys = turn_cos_sin(iota((nyp, atoms), 0).astype(f32) * y_turns)
    for m in range(2 * z_reach + 1):
        c1, s1 = zc[m : m + 1], zs[m : m + 1]
        xz[0, m * nx : (m + 1) * nx, :] = xc * c1 - xs * s1
        xz[1, m * nx : (m + 1) * nx, :] = xc * s1 + xs * c1
    ymat[...] = jnp.zeros_like(ymat)
    rise = iota((nyp, atoms), 0).astype(f32) * (two_pi / yz)
    for half in range(2):
        cut = slice(half * atoms, (half + 1) * atoms)
        far = slice((2 + half) * atoms, (3 + half) * atoms)
        sign = -1.0 if half == 0 else 1.0
        base = 2 * half * nyp
        ymat[base : base + nyp, cut] = yc
        ymat[base + nyp : base + 2 * nyp, cut] = ys
        ymat[base : base + nyp, far] = sign * rise * ys
        ymat[base + nyp : base + 2 * nyp, far] = -sign * rise * yc
    high, low = split(ymat[...])
    ypair[:width_y, :] = high
    ypair[width_y:, :] = low

    arrive(spread_copies)
    pieces[...] = (
        mm(route, spread[...].reshape(atoms, width)).astype(bf16).reshape(yz, blocks, piece, width)
    )
    piece_copies = start(
        [to_yz(pieces.at[peer(k)], work.at[:, me], pc_s.at[k], pc_r.at[k], k) for k in others]
    )
    work[:, pl.ds(me, 1)] = pieces[me].reshape(blocks, 1, piece, width)

    arrive(ghost_copies)
    part = iota((8, 4 * halos), 1) // halos
    lead = iota((8, 4 * halos), 0)
    ghosts = jnp.zeros((8, 4 * halos), f32)
    for i, (axis, shift) in enumerate(((0, -1.0), (0, 1.0), (1, -1.0), (1, 1.0))):
        ghosts = jnp.where(part == i, ghost_pos[i] + jnp.where(lead == axis, shift, 0.0), ghosts)
    table_pos = jnp.concatenate([meta, ghosts], axis=1)
    table = table_pos.shape[1]
    nrad = rin.shape[0]
    centres = iota((2 * nrad, atoms), 0).astype(f32) * (cutoff_radius / (nrad - 1))

    halfway = groups // 2

    def emit(g, begin=0, end=group):
        for s in range(begin, end):
            radials[g, s] = mm(rout_t, hidden[g, s]).astype(bf16)

    hidden[0] = jnp.zeros_like(hidden[0])

    def radial_step(g, carry):
        index = nbr[pl.ds(pl.multiple_of(g * group, group), group), :]
        local_index = index % lanes
        where = index // lanes
        rs = []
        for m in range(3):
            cols = []
            for h in range(atoms // lanes):
                cut = slice(h * lanes, (h + 1) * lanes)
                found = jnp.zeros((group, lanes), f32)
                for t in range(table // lanes):
                    tile = jnp.broadcast_to(
                        table_pos[m : m + 1, t * lanes : (t + 1) * lanes], (group, lanes)
                    )
                    got = jnp.take_along_axis(
                        tile, local_index[:, cut], axis=1, mode="promise_in_bounds"
                    )
                    found = jnp.where(where[:, cut] == t, got, found)
                cols.append(found)
            r = jnp.concatenate(cols, axis=1) - meta[m : m + 1]
            rel[g, m] = r
            rs.append(r)
        dist = jnp.sqrt(rs[0] * rs[0] + rs[1] * rs[1] + rs[2] * rs[2])
        u = dist * (1.0 / cutoff_radius)
        u2 = u * u
        u6 = u2 * u2 * u2
        env = 1.0 + u6 * (-28.0 + u * (48.0 - 21.0 * u))
        live = (iota((group, atoms), 0) + g * group) < counts
        env = jnp.where(live, env, 0.0)
        basis = []
        for s in range(group):
            off = dist[s : s + 1] - centres
            basis.append(jnp.exp(-basis_sharpness * off * off))
        h = mm(rin_t, jnp.concatenate(basis, axis=1).astype(bf16))
        emit(g, 0, 2)
        h = mm(mid_t[0], silu(h).astype(bf16))
        emit(g, 2, 5)
        h = mm(mid_t[1], silu(h).astype(bf16))
        emit(g, 5, group)
        h = silu(h)
        for s in range(group):
            hidden[g + 1, s] = (h[:, s * atoms : (s + 1) * atoms] * env[s : s + 1]).astype(bf16)
        return carry

    lax.fori_loop(0, halfway, radial_step, 0)

    arrive(piece_copies)
    owned = work[...].reshape(atoms, width)
    halo_feat[...] = mm(pick, owned).astype(bf16)
    halo_copies = start(
        [send(halo_feat, ghost_feat.at[i], hf_s.at[i], hf_r.at[i], k) for i, (send, k) in enumerate(ways)]
    )

    scalars = owned[:, :channels]
    q = nt(use("charge")[...], scalars)
    weighted = [
        (xz[i][:, None, :] * q[None]).reshape(pairs * latent, atoms) for i in range(2)
    ]
    high, low = split(jnp.concatenate(weighted, axis=1))
    cut = slice(0, 2 * atoms)
    wide = nt(high, ypair[:, cut])
    part_out[...] = (
        wide[:, :width_y] + wide[:, width_y:] + nt(low, ypair[:width_y, cut])
    ).reshape(yz, share, width_y)
    part_copies = start(
        [to_yz(part_out.at[peer(k)], part_got.at[k], rs_s.at[k], rs_r.at[k], k) for k in others]
    )

    up = use("up")

    def raise_rows(rows, begin, size):
        parts = [
            mm(rows[:, p * channels : (p + 1) * channels], up[min(p, 1)]).T for p in range(4)
        ]
        table_t[:, begin : begin + size] = interleave(parts).astype(bf16)

    raise_rows(owned, 0, atoms)

    skip = mm(scalars, sw[0]).T
    pulls = [
        nt(to_f, owned[:, (1 + m) * channels : (2 + m) * channels].astype(f32), highest)[0:1]
        for m in range(3)
    ]
    prod = use("prod")
    kinds = prod.shape[0]
    which = (iota((8, atoms), 0).astype(f32) == meta[3:4]).astype(f32).astype(bf16)
    weights = prod[...]
    high = weights.astype(bf16).astype(f32)
    middle = (weights - high).astype(bf16).astype(f32)
    low = weights - high - middle
    blank = jnp.zeros((8 - kinds, weights.shape[1]), f32)
    stack = jnp.concatenate([high, blank, middle, blank, low, blank], axis=0)
    p_t = tn(stack.astype(bf16), jnp.concatenate([which] * 3, axis=0))

    lax.fori_loop(halfway, groups, radial_step, 0)
    emit(groups)
    acc[...] = jnp.zeros_like(acc)
    arrive(halo_copies)
    raise_rows(jnp.concatenate([ghost_feat[i] for i in range(4)], axis=0), atoms, 4 * halos)

    def message_step(g, carry):
        for begin in range(0, group, together):
            chosen = range(begin, begin + together)
            ups = [mm(table_t[...], hots[g, s]) for s in chosen]
            rm = [
                [jnp.broadcast_to(rel[g, m, s : s + 1, :], (8, atoms)) for m in range(3)]
                for s in chosen
            ]
            for c in range(channels // 8):
                sums = [None] * 4
                for i, s in enumerate(chosen):
                    rows = ups[i][32 * c : 32 * c + 32]
                    u = [rows[8 * p : 8 * p + 8] for p in range(4)]
                    rows = radials[g + 1, s, 32 * c : 32 * c + 32, :].astype(f32)
                    rad = [rows[8 * p : 8 * p + 8] for p in range(4)]
                    x, y, z = rm[i]
                    ru = rad[2] * u[0]
                    terms = [rad[0] * u[0] + rad[1] * (x * u[1] + y * u[2] + z * u[3])]
                    terms += [ru * rm[i][m] + rad[3] * u[1 + m] for m in range(3)]
                    sums = [t if p is None else p + t for p, t in zip(sums, terms)]
                for m in range(4):
                    acc[c, m] += sums[m]
        return carry

    first, second = groups // 4, 5 * groups // 8
    lax.fori_loop(0, first, message_step, 0)

    arrive(part_copies)
    total = part_out[me]
    for k in range(1, yz):
        total = total + part_got[k]
    row_sum[...] = total
    row_copies = start(
        [to_gx(row_sum, row_got.at[k], gs_s.at[k], gs_r.at[k], k) for k in range(1, gx)]
    )

    lax.fori_loop(first, second, message_step, 0)

    arrive(row_copies)
    total = row_sum[...]
    for k in range(1, gx):
        total = total + row_got[k]
    quarters = [total[:, i * nyp : (i + 1) * nyp] for i in range(4)]
    rest = jnp.zeros((share, width_y - 4 * nyp), f32)
    both, gap = gp + gm, gp - gm
    coef[...] = jnp.concatenate(
        [
            both * quarters[0] - gap * quarters[3],
            both * quarters[1] + gap * quarters[2],
            both * quarters[2] + gap * quarters[1],
            both * quarters[3] - gap * quarters[0],
            rest,
        ],
        axis=1,
    )
    coef_copies = start(
        [to_yz(coef, coefs.at[me], ag_s.at[k], ag_r.at[k], k) for k in others]
    )
    coefs[me] = coef[...]

    lax.fori_loop(second, groups, message_step, 0)

    arrive(coef_copies)
    high, low = split(coefs[...].reshape(yz * share, width_y))
    v = mm(jnp.concatenate([high, high], axis=1), ypair[...]) + mm(low, ypair[:width_y, :])
    v_re, v_im, y_im, y_re = [v[:, i * atoms : (i + 1) * atoms] for i in range(4)]
    zero = jnp.zeros((latent, atoms), f32)
    potential, field = zero, [zero, zero, zero]
    for j in range(pairs):
        cut = slice(j * latent, (j + 1) * latent)
        cos_row, sin_row = xz[0, j : j + 1], xz[1, j : j + 1]
        d_im = cos_row * v_im[cut] - sin_row * v_re[cut]
        potential = potential + (cos_row * v_re[cut] + sin_row * v_im[cut])
        field[0] = field[0] - ((j % nx) + 1) * (two_pi / gx) * d_im
        field[1] = field[1] - (cos_row * y_im[cut] - sin_row * y_re[cut])
        field[2] = field[2] - ((j // nx) - z_reach) * two_pi * d_im

    scale = 1.0 / math.sqrt(slots)
    p = [p_t[i * channels : (i + 1) * channels] for i in range(5)]
    a0 = acc[:, 0].reshape(channels, atoms) * scale
    a1 = [acc[:, 1 + m].reshape(channels, atoms) * scale for m in range(3)]
    square = a1[0] * a1[0] + a1[1] * a1[1] + a1[2] * a1[2]
    b0 = (p[0] * a0 + p[1] * a0 * a0 + p[2] * square).astype(bf16)
    b1 = [(p[3] * a1[m] + p[4] * a0 * a1[m]).astype(bf16) for m in range(3)]
    scal = tn(ow[0], b0) + skip + tn(use("fieldw")[...], potential, highest)
    readout = silu(mm(use("readw")[...], scal.astype(bf16)))
    rvec = use("rvec")
    tall = jnp.broadcast_to(rvec[...], (8, rvec.shape[1]))
    energy = mm(tall, readout, highest)[0:1] + 0.5 * jnp.sum(q * potential, axis=0, keepdims=True)
    rows = []
    for m in range(3):
        rows.append(
            mm(to_b, b1[m].astype(f32), highest)[0:1]
            + pulls[m]
            + jnp.sum(q * field[m], axis=0, keepdims=True)
        )
    result = jnp.concatenate(rows + [energy, jnp.zeros((4, atoms), f32)], axis=0)
    for k in range(yz):
        for b in range(blocks):
            cut = slice(b * block, (b + 1) * block)
            code = meta_got[k, 4:5, cut]
            total = jnp.zeros((8, block), f32)
            for s in range(blocks):
                mine = (me * blocks + s).astype(f32)
                total = total + jnp.where(
                    code == mine, result[:, s * block : (s + 1) * block], 0.0
                )
            back[k, :, cut] = total
    back_copies = start(
        [to_yz(back.at[k], came.at[k], ret_s.at[k], ret_r.at[k], yz - k) for k in others]
    )
    arrive(back_copies)
    total = back[0]
    for k in range(1, yz):
        total = total + came[k]
    out[...] = total
    for c in sent:
        c.wait_send()
    assert not loads


def home_kernel(results, forces, energies):
    forces[...] = results[:3]
    energies[...] = results[3:4]


def on_device(
    positions,
    species,
    features,
    move_dest,
    move_slot,
    halo_list,
    neighbours,
    neighbour_count,
    wave_index,
    radial_in,
    radial_mid,
    radial_out,
    up_weight,
    prod_weight,
    out_weight,
    skip_weight,
    charge_weight,
    field_weight,
    read_weight,
    read_vector,
    force_weight,
):
    gx, yz = lax.axis_size("gx"), lax.axis_size("yz")
    atoms, width = features.shape
    blocks = move_dest.shape[0]
    piece = atoms // blocks // yz
    slots = neighbours.shape[1]
    channels = width // 4
    latent = charge_weight.shape[1]
    nyp = -(-(2 * yz + 1) // 8) * 8
    pairs = 2 * gx * (2 * z_reach + 1)
    share = pairs * latent // yz
    wide = -(-4 * nyp // lanes) * lanes
    halo = halo_list.shape[0]
    groups = slots // group
    table = atoms + 4 * halo
    hidden = radial_mid.shape[1]

    given = {
        "dest": move_dest.reshape(1, -1),
        "slot": move_slot.reshape(1, -1),
        "pos": positions,
        "species": species.reshape(1, -1),
        "feat": features.reshape(blocks, yz, piece, width),
        "halo": halo_list.reshape(1, -1),
        "wave": wave_index,
        "nbr": neighbours.T,
        "count": neighbour_count.reshape(1, -1),
        "rin": radial_in,
        "mid": radial_mid,
        "rout": radial_out,
        "up": up_weight,
        "prod": prod_weight,
        "ow": out_weight,
        "sw": skip_weight,
        "charge": charge_weight.T,
        "fieldw": field_weight,
        "readw": read_weight.T,
        "rvec": read_vector.reshape(1, -1),
        "fw": force_weight.reshape(1, -1),
    }

    def dma(n):
        return [pltpu.SemaphoreType.DMA((n,)), pltpu.SemaphoreType.DMA((n,))]

    scratch = [pltpu.VMEM(given[name].shape, given[name].dtype) for name in fields]
    scratch += [
        pltpu.VMEM((8, atoms), f32),
        pltpu.VMEM((yz, 8, atoms), f32),
        pltpu.VMEM((yz, blocks, piece, width), bf16),
        pltpu.VMEM((yz, blocks, piece, width), bf16),
        pltpu.VMEM((blocks, yz, piece, width), bf16),
        pltpu.VMEM((8, 4 * halo), f32),
        pltpu.VMEM((4, 8, 4 * halo), f32),
        pltpu.VMEM((halo, width), bf16),
        pltpu.VMEM((4, halo, width), bf16),
        pltpu.VMEM((2, pairs, atoms), f32),
        pltpu.VMEM((wide, 4 * atoms), f32),
        pltpu.VMEM((2 * wide, 4 * atoms), bf16),
        pltpu.VMEM((yz, share, wide), f32),
        pltpu.VMEM((yz, share, wide), f32),
        pltpu.VMEM((share, wide), f32),
        pltpu.VMEM((gx, share, wide), f32),
        pltpu.VMEM((share, wide), f32),
        pltpu.VMEM((yz, share, wide), f32),
        pltpu.VMEM((groups, 3, group, atoms), f32),
        pltpu.VMEM((groups + 1, group, hidden, atoms), bf16),
        pltpu.VMEM((groups + 1, group, width, atoms), bf16),
        pltpu.VMEM((groups, group, table, atoms), bf16),
        pltpu.VMEM((width, table), bf16),
        pltpu.VMEM((channels // 8, 4, 8, atoms), f32),
        pltpu.VMEM((yz, 8, atoms), f32),
        pltpu.VMEM((yz, 8, atoms), f32),
    ]
    scratch += [pltpu.SemaphoreType.DMA((len(fields),))]
    scratch += dma(yz) + dma(yz) + dma(yz) + dma(4) + dma(4) + dma(yz) + dma(gx) + dma(yz) + dma(yz)
    results = pl.pallas_call(
        functools.partial(step_kernel, (gx, yz, nyp)),
        out_shape=jax.ShapeDtypeStruct((8, atoms), f32),
        in_specs=[pl.BlockSpec(memory_space=pl.ANY)] * len(fields),
        out_specs=VMEM,
        scratch_shapes=scratch,
        compiler_params=pltpu.CompilerParams(
            collective_id=0, has_side_effects=True, vmem_limit_bytes=56 * 1024 * 1024
        ),
    )(*[given[name] for name in fields])
    forces, energies = pl.pallas_call(
        home_kernel,
        out_shape=[
            jax.ShapeDtypeStruct((3, atoms), f32),
            jax.ShapeDtypeStruct((1, atoms), f32),
        ],
        in_specs=[VMEM],
        out_specs=[VMEM, VMEM],
    )(results)
    return forces, energies.reshape(atoms)


def solution(mesh):
    split = P(("gx", "yz"))
    rows = P(("gx", "yz"), None)
    in_specs = (P(None, ("gx", "yz")), split, rows, split, split, split, rows, split) + (P(),) * 13
    out_specs = (P(None, ("gx", "yz")), split)
    return jax.shard_map(
        on_device, mesh=mesh, in_specs=in_specs, out_specs=out_specs, check_vma=False
    )
```

```python
import functools
import math

import jax
import jax.numpy as jnp
from jax import lax
from jax.experimental import pallas as pl
from jax.experimental.pallas import tpu as pltpu
from jax.sharding import PartitionSpec as P

highest = lax.Precision.HIGHEST
two_pi = 2.0 * math.pi
cutoff_radius = 3.5
basis_sharpness = 4.0
ewald_width = 0.1
ewald_scale = 0.01
z_reach = 2
lanes = 128
group = 8
together = 2
f32 = jnp.float32
bf16 = jnp.bfloat16
i32 = jnp.int32

VMEM = pl.BlockSpec(memory_space=pltpu.VMEM)
MESH = pl.DeviceIdType.MESH
NT = (((1,), (1,)), ((), ()))
TN = (((0,), (0,)), ((), ()))


def nt(a, b, precision=None):
    return lax.dot_general(a, b, NT, precision=precision, preferred_element_type=f32)


def tn(a, b, precision=None):
    return lax.dot_general(a, b, TN, precision=precision, preferred_element_type=f32)


def mm(a, b, precision=None):
    return jnp.dot(a, b, precision=precision, preferred_element_type=f32)


def iota(shape, dim):
    return lax.broadcasted_iota(jnp.int32, shape, dim)


def silu(v):
    half = 0.5 * v
    return half + half * jnp.tanh(half)


def turn_cos_sin(turns):
    frac = turns - jnp.floor(turns + 0.5)
    angle = two_pi * frac
    return jnp.cos(angle), jnp.sin(angle)


def flip(a):
    return a.astype(f32).T.astype(a.dtype)


def split(a):
    high = a.astype(bf16)
    return high, (a - high.astype(f32)).astype(bf16)


def interleave(parts):
    tall = parts[0].shape[0]
    return jnp.concatenate([p[c : c + 8] for c in range(0, tall, 8) for p in parts], axis=0)


fields = (
    "dest", "slot", "pos", "species", "feat", "halo", "wave", "nbr", "count", "rin", "mid",
    "rout", "up", "prod", "ow", "sw", "charge", "fieldw", "readw", "rvec", "fw",
)


def step_kernel(sizes, *refs):
    gx, yz, nyp = sizes
    n_in = len(fields)
    sources, refs = refs[:n_in], refs[n_in:]
    out, refs = refs[0], refs[1:]
    local, refs = dict(zip(fields, refs[:n_in])), refs[n_in:]
    (
        meta_in, meta_got, spread, pieces, work, halo_pos, ghost_pos, halo_feat, ghost_feat,
        xz, ymat, ypair, part_out, part_got, row_sum, row_got, coef, coefs,
        rel, hidden, radials, hots, table_t, acc, back, came,
        in_s, meta_s, meta_r, sp_s, sp_r, pc_s, pc_r, hp_s, hp_r, hf_s, hf_r, rs_s, rs_r,
        gs_s, gs_r, ag_s, ag_r, ret_s, ret_r,
    ) = refs
    row, me = lax.axis_index("gx"), lax.axis_index("yz")
    blocks, parts, piece, width = local["feat"].shape
    channels = width // 4
    block = parts * piece
    atoms = blocks * block
    slots = local["nbr"].shape[0]
    groups = slots // group
    latent = local["charge"].shape[0]
    nx = 2 * gx
    pairs = nx * (2 * z_reach + 1)
    share = pairs * latent // yz
    halos = local["halo"].shape[1]
    width_y = ymat.shape[0]

    def peer(k):
        return lax.rem(me + k, yz)

    def row_peer(k):
        return lax.rem(row + k, gx)

    def to_yz(src, dst, s, r, k):
        return pltpu.make_async_remote_copy(
            src_ref=src, dst_ref=dst, send_sem=s, recv_sem=r,
            device_id={"yz": peer(k)}, device_id_type=MESH,
        )

    def to_gx(src, dst, s, r, k):
        return pltpu.make_async_remote_copy(
            src_ref=src, dst_ref=dst, send_sem=s, recv_sem=r,
            device_id={"gx": row_peer(k)}, device_id_type=MESH,
        )

    barrier = pltpu.get_barrier_semaphore()
    for k in range(1, yz):
        pl.semaphore_signal(barrier, inc=1, device_id={"yz": peer(k)}, device_id_type=MESH)
    for k in range(1, gx):
        pl.semaphore_signal(barrier, inc=1, device_id={"gx": row_peer(k)}, device_id_type=MESH)
    loads = {}
    for i, name in enumerate(fields):
        loads[name] = pltpu.make_async_copy(sources[i], local[name], in_s.at[i])
        loads[name].start()

    def use(name):
        if name in loads:
            loads.pop(name).wait()
        return local[name]

    dest, slot = use("dest"), use("slot")
    lane = iota((1, atoms), 1)
    place = jnp.zeros((1, atoms), i32)
    spot = jnp.zeros((1, atoms), i32)
    for b in range(blocks):
        code = dest[:, b : b + 1] * blocks + slot[:, b : b + 1]
        place = jnp.where(lane // block == b, code, place)
        spot = jnp.where(lane // piece == me * blocks + b, code * piece + lane % piece, spot)
    meta_in[...] = jnp.concatenate(
        [
            use("pos")[...].astype(f32),
            use("species")[...].astype(f32),
            place.astype(f32),
            spot.astype(f32),
            jnp.zeros((2, atoms), f32),
        ],
        axis=0,
    )
    feat = use("feat")
    pl.semaphore_wait(barrier, yz - 1 + gx - 1)

    sent = []

    def start(copies):
        for c in copies:
            c.start()
        sent.extend(copies)
        return copies

    def arrive(copies):
        for c in copies:
            c.wait_recv()

    others = range(1, yz)
    meta_copies = start(
        [to_yz(meta_in, meta_got.at[k], meta_s.at[k], meta_r.at[k], k) for k in others]
    )
    spread_copies = start(
        [to_yz(feat.at[:, peer(k)], spread.at[me], sp_s.at[k], sp_r.at[k], k) for k in others]
    )

    spread[me] = feat[:, pl.ds(me, 1)].reshape(blocks, piece, width)
    meta_got[0] = meta_in[...]
    wave = use("wave")
    codes = (wave[2:3, :] + z_reach) * nx + wave[0:1, :] - 1
    waves = wave.shape[1]
    hot = ((me * share + iota((share, waves), 0)) // latent == codes).astype(f32).astype(bf16)
    level = iota((nyp, waves), 0)
    plus = (level == wave[1:2, :]).astype(f32).astype(bf16)
    minus = ((level == -wave[1:2, :]) & (level > 0)).astype(f32).astype(bf16)
    pair = (me * share + iota((share, nyp), 0)) // latent
    wx = ((pair % nx) + 1).astype(f32) * (two_pi / gx)
    wz = ((pair // nx) - z_reach).astype(f32) * two_pi
    wy = iota((share, nyp), 1).astype(f32) * (two_pi / yz)
    squared = wx * wx + wy * wy + wz * wz
    prefactor = 8.0 * math.pi * ewald_scale / (gx * yz)
    weight = prefactor * jnp.exp(-0.5 * ewald_width * ewald_width * squared) / squared
    gp, gm = weight * nt(hot, plus), weight * nt(hot, minus)
    rin = use("rin")
    rin_t = jnp.concatenate([rin[...].astype(f32), jnp.zeros_like(rin, f32)], axis=0).T.astype(bf16)
    mid = use("mid")
    mid_t = [flip(mid[i]) for i in range(2)]
    tall = use("rout")[...].astype(f32).T
    rout_t = interleave([tall[p * channels : (p + 1) * channels] for p in range(4)]).astype(bf16)
    list4 = jnp.concatenate([use("halo")[...]] * 4, axis=1)
    pick_t = (iota((atoms, 4 * halos), 0) == list4).astype(f32)
    pick = pick_t.T[:halos].astype(bf16)
    force8 = jnp.broadcast_to(use("fw")[...], (8, channels))
    ow, sw = use("ow"), use("sw")
    to_b = nt(force8, ow[1].astype(f32), highest)
    to_f = nt(force8, sw[1].astype(f32), highest)
    nbr, counts = use("nbr"), use("count")[...]

    packed = 16
    base = iota((packed, atoms), 0).astype(f32).astype(bf16)
    one, nil = jnp.ones((packed, atoms), bf16), jnp.zeros((packed, atoms), bf16)

    def hot_of(index):
        near = jnp.broadcast_to(index, (packed, atoms)).astype(f32)
        far = (near - atoms).astype(bf16)
        near = near.astype(bf16)
        tiles = [jnp.where(near - t == base, one, nil) for t in range(0, atoms, packed)]
        tiles += [jnp.where(far - t == base, one, nil) for t in range(0, 4 * halos, packed)]
        return jnp.concatenate(tiles, axis=0)

    def hot_step(g, carry):
        index = nbr[pl.ds(pl.multiple_of(g * group, group), group), :]
        for s in range(group):
            hots[g, s] = hot_of(index[s : s + 1])
        return carry

    lax.fori_loop(0, groups, hot_step, 0)

    arrive(meta_copies)
    metas = []
    for s in range(blocks):
        mine = (me * blocks + s).astype(f32)
        total = jnp.zeros((8, block), f32)
        for k in range(yz):
            for b in range(blocks):
                got = meta_got[k, :, b * block : (b + 1) * block]
                total = total + jnp.where(got[4:5, :] == mine, got, 0.0)
        metas.append(total)
    meta = jnp.concatenate(metas, axis=1)
    halo_pos[...] = mm(meta.astype(bf16), pick_t.astype(bf16))
    ways = ((to_gx, 1), (to_gx, gx - 1), (to_yz, 1), (to_yz, yz - 1))
    ghost_copies = start(
        [send(halo_pos, ghost_pos.at[i], hp_s.at[i], hp_r.at[i], k) for i, (send, k) in enumerate(ways)]
    )
    targets = meta_got[0, 5:6, :]
    for k in range(1, yz):
        targets = targets + meta_got[k, 5:6, :]
    route = (iota((atoms, atoms), 0).astype(f32) == targets).astype(f32).astype(bf16)

    x_turns = (meta[0:1] + row.astype(f32)) * (1.0 / gx)
    y_turns = (meta[1:2] + me.astype(f32)) * (1.0 / yz)
    xc, xs = turn_cos_sin((iota((nx, atoms), 0) + 1).astype(f32) * x_turns)
    zc, zs = turn_cos_sin((iota((8, atoms), 0) - z_reach).astype(f32) * meta[2:3])
    yc, ys = turn_cos_sin(iota((nyp, atoms), 0).astype(f32) * y_turns)
    for m in range(2 * z_reach + 1):
        c1, s1 = zc[m : m + 1], zs[m : m + 1]
        xz[0, m * nx : (m + 1) * nx, :] = xc * c1 - xs * s1
        xz[1, m * nx : (m + 1) * nx, :] = xc * s1 + xs * c1
    ymat[...] = jnp.zeros_like(ymat)
    rise = iota((nyp, atoms), 0).astype(f32) * (two_pi / yz)
    for half in range(2):
        cut = slice(half * atoms, (half + 1) * atoms)
        far = slice((2 + half) * atoms, (3 + half) * atoms)
        sign = -1.0 if half == 0 else 1.0
        base = 2 * half * nyp
        ymat[base : base + nyp, cut] = yc
        ymat[base + nyp : base + 2 * nyp, cut] = ys
        ymat[base : base + nyp, far] = sign * rise * ys
        ymat[base + nyp : base + 2 * nyp, far] = -sign * rise * yc
    high, low = split(ymat[...])
    ypair[:width_y, :] = high
    ypair[width_y:, :] = low

    arrive(spread_copies)
    pieces[...] = (
        mm(route, spread[...].reshape(atoms, width)).astype(bf16).reshape(yz, blocks, piece, width)
    )
    piece_copies = start(
        [to_yz(pieces.at[peer(k)], work.at[:, me], pc_s.at[k], pc_r.at[k], k) for k in others]
    )
    work[:, pl.ds(me, 1)] = pieces[me].reshape(blocks, 1, piece, width)

    prod = use("prod")
    kinds = prod.shape[0]
    which = (iota((8, atoms), 0).astype(f32) == meta[3:4]).astype(f32).astype(bf16)
    weights = prod[...]
    high = weights.astype(bf16).astype(f32)
    middle = (weights - high).astype(bf16).astype(f32)
    low = weights - high - middle
    blank = jnp.zeros((8 - kinds, weights.shape[1]), f32)
    stack = jnp.concatenate([high, blank, middle, blank, low, blank], axis=0)
    p_t = tn(stack.astype(bf16), jnp.concatenate([which] * 3, axis=0))
    acc[...] = jnp.zeros_like(acc)
    hidden[0] = jnp.zeros_like(hidden[0])
    arrive(ghost_copies)
    part = iota((8, 4 * halos), 1) // halos
    lead = iota((8, 4 * halos), 0)
    ghosts = jnp.zeros((8, 4 * halos), f32)
    for i, (axis, shift) in enumerate(((0, -1.0), (0, 1.0), (1, -1.0), (1, 1.0))):
        ghosts = jnp.where(part == i, ghost_pos[i] + jnp.where(lead == axis, shift, 0.0), ghosts)
    table_pos = jnp.concatenate([meta, ghosts], axis=1)
    table = table_pos.shape[1]
    nrad = rin.shape[0]
    centres = iota((2 * nrad, atoms), 0).astype(f32) * (cutoff_radius / (nrad - 1))

    halfway = groups // 2

    def emit(g, begin=0, end=group):
        for s in range(begin, end):
            radials[g, s] = mm(rout_t, hidden[g, s]).astype(bf16)


    def radial_step(g, carry):
        index = nbr[pl.ds(pl.multiple_of(g * group, group), group), :]
        local_index = index % lanes
        where = index // lanes
        rs = []
        for m in range(3):
            cols = []
            for h in range(atoms // lanes):
                cut = slice(h * lanes, (h + 1) * lanes)
                found = jnp.zeros((group, lanes), f32)
                for t in range(table // lanes):
                    tile = jnp.broadcast_to(
                        table_pos[m : m + 1, t * lanes : (t + 1) * lanes], (group, lanes)
                    )
                    got = jnp.take_along_axis(
                        tile, local_index[:, cut], axis=1, mode="promise_in_bounds"
                    )
                    found = jnp.where(where[:, cut] == t, got, found)
                cols.append(found)
            r = jnp.concatenate(cols, axis=1) - meta[m : m + 1]
            rel[g, m] = r
            rs.append(r)
        dist = jnp.sqrt(rs[0] * rs[0] + rs[1] * rs[1] + rs[2] * rs[2])
        u = dist * (1.0 / cutoff_radius)
        u2 = u * u
        u6 = u2 * u2 * u2
        env = 1.0 + u6 * (-28.0 + u * (48.0 - 21.0 * u))
        live = (iota((group, atoms), 0) + g * group) < counts
        env = jnp.where(live, env, 0.0)
        basis = []
        for s in range(group):
            off = dist[s : s + 1] - centres
            basis.append(jnp.exp(-basis_sharpness * off * off))
        h = mm(rin_t, jnp.concatenate(basis, axis=1).astype(bf16))
        emit(g, 0, 2)
        h = mm(mid_t[0], silu(h).astype(bf16))
        emit(g, 2, 5)
        h = mm(mid_t[1], silu(h).astype(bf16))
        emit(g, 5, group)
        h = silu(h)
        for s in range(group):
            hidden[g + 1, s] = (h[:, s * atoms : (s + 1) * atoms] * env[s : s + 1]).astype(bf16)
        return carry

    lax.fori_loop(0, halfway, radial_step, 0)

    arrive(piece_copies)
    owned = work[...].reshape(atoms, width)
    halo_feat[...] = mm(pick, owned).astype(bf16)
    halo_copies = start(
        [send(halo_feat, ghost_feat.at[i], hf_s.at[i], hf_r.at[i], k) for i, (send, k) in enumerate(ways)]
    )

    scalars = owned[:, :channels]
    q = nt(use("charge")[...], scalars)
    weighted = [
        (xz[i][:, None, :] * q[None]).reshape(pairs * latent, atoms) for i in range(2)
    ]
    high, low = split(jnp.concatenate(weighted, axis=1))
    cut = slice(0, 2 * atoms)
    wide = nt(high, ypair[:, cut])
    part_out[...] = (
        wide[:, :width_y] + wide[:, width_y:] + nt(low, ypair[:width_y, cut])
    ).reshape(yz, share, width_y)
    part_copies = start(
        [to_yz(part_out.at[peer(k)], part_got.at[k], rs_s.at[k], rs_r.at[k], k) for k in others]
    )

    up = use("up")

    def raise_rows(rows, begin, size):
        parts = [
            mm(rows[:, p * channels : (p + 1) * channels], up[min(p, 1)]).T for p in range(4)
        ]
        table_t[:, begin : begin + size] = interleave(parts).astype(bf16)

    raise_rows(owned, 0, atoms)

    skip = mm(scalars, sw[0]).T
    pulls = [
        nt(to_f, owned[:, (1 + m) * channels : (2 + m) * channels].astype(f32), highest)[0:1]
        for m in range(3)
    ]

    lax.fori_loop(halfway, groups, radial_step, 0)
    emit(groups)
    arrive(halo_copies)
    raise_rows(jnp.concatenate([ghost_feat[i] for i in range(4)], axis=0), atoms, 4 * halos)

    def message_step(g, carry):
        for begin in range(0, group, together):
            chosen = range(begin, begin + together)
            ups = [mm(table_t[...], hots[g, s]) for s in chosen]
            rm = [
                [jnp.broadcast_to(rel[g, m, s : s + 1, :], (8, atoms)) for m in range(3)]
                for s in chosen
            ]
            for c in range(channels // 8):
                sums = [None] * 4
                for i, s in enumerate(chosen):
                    rows = ups[i][32 * c : 32 * c + 32]
                    u = [rows[8 * p : 8 * p + 8] for p in range(4)]
                    rows = radials[g + 1, s, 32 * c : 32 * c + 32, :].astype(f32)
                    rad = [rows[8 * p : 8 * p + 8] for p in range(4)]
                    x, y, z = rm[i]
                    ru = rad[2] * u[0]
                    terms = [rad[0] * u[0] + rad[1] * (x * u[1] + y * u[2] + z * u[3])]
                    terms += [ru * rm[i][m] + rad[3] * u[1 + m] for m in range(3)]
                    sums = [t if p is None else p + t for p, t in zip(sums, terms)]
                for m in range(4):
                    acc[c, m] += sums[m]
        return carry

    first, second = groups // 4, 5 * groups // 8
    lax.fori_loop(0, first, message_step, 0)

    arrive(part_copies)
    total = part_out[me]
    for k in range(1, yz):
        total = total + part_got[k]
    row_sum[...] = total
    row_copies = start(
        [to_gx(row_sum, row_got.at[k], gs_s.at[k], gs_r.at[k], k) for k in range(1, gx)]
    )

    lax.fori_loop(first, second, message_step, 0)

    arrive(row_copies)
    total = row_sum[...]
    for k in range(1, gx):
        total = total + row_got[k]
    quarters = [total[:, i * nyp : (i + 1) * nyp] for i in range(4)]
    rest = jnp.zeros((share, width_y - 4 * nyp), f32)
    both, gap = gp + gm, gp - gm
    coef[...] = jnp.concatenate(
        [
            both * quarters[0] - gap * quarters[3],
            both * quarters[1] + gap * quarters[2],
            both * quarters[2] + gap * quarters[1],
            both * quarters[3] - gap * quarters[0],
            rest,
        ],
        axis=1,
    )
    coef_copies = start(
        [to_yz(coef, coefs.at[me], ag_s.at[k], ag_r.at[k], k) for k in others]
    )
    coefs[me] = coef[...]

    lax.fori_loop(second, groups, message_step, 0)

    arrive(coef_copies)
    high, low = split(coefs[...].reshape(yz * share, width_y))
    v = mm(jnp.concatenate([high, high], axis=1), ypair[...]) + mm(low, ypair[:width_y, :])
    v_re, v_im, y_im, y_re = [v[:, i * atoms : (i + 1) * atoms] for i in range(4)]
    zero = jnp.zeros((latent, atoms), f32)
    potential, field = zero, [zero, zero, zero]
    for j in range(pairs):
        cut = slice(j * latent, (j + 1) * latent)
        cos_row, sin_row = xz[0, j : j + 1], xz[1, j : j + 1]
        d_im = cos_row * v_im[cut] - sin_row * v_re[cut]
        potential = potential + (cos_row * v_re[cut] + sin_row * v_im[cut])
        field[0] = field[0] - ((j % nx) + 1) * (two_pi / gx) * d_im
        field[1] = field[1] - (cos_row * y_im[cut] - sin_row * y_re[cut])
        field[2] = field[2] - ((j // nx) - z_reach) * two_pi * d_im

    scale = 1.0 / math.sqrt(slots)
    p = [p_t[i * channels : (i + 1) * channels] for i in range(5)]
    a0 = acc[:, 0].reshape(channels, atoms) * scale
    a1 = [acc[:, 1 + m].reshape(channels, atoms) * scale for m in range(3)]
    square = a1[0] * a1[0] + a1[1] * a1[1] + a1[2] * a1[2]
    b0 = (p[0] * a0 + p[1] * a0 * a0 + p[2] * square).astype(bf16)
    b1 = [(p[3] * a1[m] + p[4] * a0 * a1[m]).astype(bf16) for m in range(3)]
    scal = tn(ow[0], b0) + skip + tn(use("fieldw")[...], potential, highest)
    readout = silu(mm(use("readw")[...], scal.astype(bf16)))
    rvec = use("rvec")
    tall = jnp.broadcast_to(rvec[...], (8, rvec.shape[1]))
    energy = mm(tall, readout, highest)[0:1] + 0.5 * jnp.sum(q * potential, axis=0, keepdims=True)
    rows = []
    for m in range(3):
        rows.append(
            mm(to_b, b1[m].astype(f32), highest)[0:1]
            + pulls[m]
            + jnp.sum(q * field[m], axis=0, keepdims=True)
        )
    result = jnp.concatenate(rows + [energy, jnp.zeros((4, atoms), f32)], axis=0)
    for k in range(yz):
        for b in range(blocks):
            cut = slice(b * block, (b + 1) * block)
            code = meta_got[k, 4:5, cut]
            total = jnp.zeros((8, block), f32)
            for s in range(blocks):
                mine = (me * blocks + s).astype(f32)
                total = total + jnp.where(
                    code == mine, result[:, s * block : (s + 1) * block], 0.0
                )
            back[k, :, cut] = total
    back_copies = start(
        [to_yz(back.at[k], came.at[k], ret_s.at[k], ret_r.at[k], yz - k) for k in others]
    )
    arrive(back_copies)
    total = back[0]
    for k in range(1, yz):
        total = total + came[k]
    out[...] = total
    for c in sent:
        c.wait_send()
    assert not loads


def home_kernel(results, forces, energies):
    forces[...] = results[:3]
    energies[...] = results[3:4]


def on_device(
    positions,
    species,
    features,
    move_dest,
    move_slot,
    halo_list,
    neighbours,
    neighbour_count,
    wave_index,
    radial_in,
    radial_mid,
    radial_out,
    up_weight,
    prod_weight,
    out_weight,
    skip_weight,
    charge_weight,
    field_weight,
    read_weight,
    read_vector,
    force_weight,
):
    gx, yz = lax.axis_size("gx"), lax.axis_size("yz")
    atoms, width = features.shape
    blocks = move_dest.shape[0]
    piece = atoms // blocks // yz
    slots = neighbours.shape[1]
    channels = width // 4
    latent = charge_weight.shape[1]
    nyp = -(-(2 * yz + 1) // 8) * 8
    pairs = 2 * gx * (2 * z_reach + 1)
    share = pairs * latent // yz
    wide = -(-4 * nyp // lanes) * lanes
    halo = halo_list.shape[0]
    groups = slots // group
    table = atoms + 4 * halo
    hidden = radial_mid.shape[1]

    given = {
        "dest": move_dest.reshape(1, -1),
        "slot": move_slot.reshape(1, -1),
        "pos": positions,
        "species": species.reshape(1, -1),
        "feat": features.reshape(blocks, yz, piece, width),
        "halo": halo_list.reshape(1, -1),
        "wave": wave_index,
        "nbr": neighbours.T,
        "count": neighbour_count.reshape(1, -1),
        "rin": radial_in,
        "mid": radial_mid,
        "rout": radial_out,
        "up": up_weight,
        "prod": prod_weight,
        "ow": out_weight,
        "sw": skip_weight,
        "charge": charge_weight.T,
        "fieldw": field_weight,
        "readw": read_weight.T,
        "rvec": read_vector.reshape(1, -1),
        "fw": force_weight.reshape(1, -1),
    }

    def dma(n):
        return [pltpu.SemaphoreType.DMA((n,)), pltpu.SemaphoreType.DMA((n,))]

    scratch = [pltpu.VMEM(given[name].shape, given[name].dtype) for name in fields]
    scratch += [
        pltpu.VMEM((8, atoms), f32),
        pltpu.VMEM((yz, 8, atoms), f32),
        pltpu.VMEM((yz, blocks, piece, width), bf16),
        pltpu.VMEM((yz, blocks, piece, width), bf16),
        pltpu.VMEM((blocks, yz, piece, width), bf16),
        pltpu.VMEM((8, 4 * halo), f32),
        pltpu.VMEM((4, 8, 4 * halo), f32),
        pltpu.VMEM((halo, width), bf16),
        pltpu.VMEM((4, halo, width), bf16),
        pltpu.VMEM((2, pairs, atoms), f32),
        pltpu.VMEM((wide, 4 * atoms), f32),
        pltpu.VMEM((2 * wide, 4 * atoms), bf16),
        pltpu.VMEM((yz, share, wide), f32),
        pltpu.VMEM((yz, share, wide), f32),
        pltpu.VMEM((share, wide), f32),
        pltpu.VMEM((gx, share, wide), f32),
        pltpu.VMEM((share, wide), f32),
        pltpu.VMEM((yz, share, wide), f32),
        pltpu.VMEM((groups, 3, group, atoms), f32),
        pltpu.VMEM((groups + 1, group, hidden, atoms), bf16),
        pltpu.VMEM((groups + 1, group, width, atoms), bf16),
        pltpu.VMEM((groups, group, table, atoms), bf16),
        pltpu.VMEM((width, table), bf16),
        pltpu.VMEM((channels // 8, 4, 8, atoms), f32),
        pltpu.VMEM((yz, 8, atoms), f32),
        pltpu.VMEM((yz, 8, atoms), f32),
    ]
    scratch += [pltpu.SemaphoreType.DMA((len(fields),))]
    scratch += dma(yz) + dma(yz) + dma(yz) + dma(4) + dma(4) + dma(yz) + dma(gx) + dma(yz) + dma(yz)
    results = pl.pallas_call(
        functools.partial(step_kernel, (gx, yz, nyp)),
        out_shape=jax.ShapeDtypeStruct((8, atoms), f32),
        in_specs=[pl.BlockSpec(memory_space=pl.ANY)] * len(fields),
        out_specs=VMEM,
        scratch_shapes=scratch,
        compiler_params=pltpu.CompilerParams(
            collective_id=0, has_side_effects=True, vmem_limit_bytes=56 * 1024 * 1024
        ),
    )(*[given[name] for name in fields])
    forces, energies = pl.pallas_call(
        home_kernel,
        out_shape=[
            jax.ShapeDtypeStruct((3, atoms), f32),
            jax.ShapeDtypeStruct((1, atoms), f32),
        ],
        in_specs=[VMEM],
        out_specs=[VMEM, VMEM],
    )(results)
    return forces, energies.reshape(atoms)


def solution(mesh):
    split = P(("gx", "yz"))
    rows = P(("gx", "yz"), None)
    in_specs = (P(None, ("gx", "yz")), split, rows, split, split, split, rows, split) + (P(),) * 13
    out_specs = (P(None, ("gx", "yz")), split)
    return jax.shard_map(
        on_device, mesh=mesh, in_specs=in_specs, out_specs=out_specs, check_vma=False
    )
```
